128 devices in a mesh: member: 2 (over x_lo), fsdp: 64 (over z, y, x_hi, core).
Axes of the slice: x: 4 (x_hi: 2, x_lo: 2; x = x_hi * 2 + x_lo), y: 4, z: 4, core: 2. Of those that a mesh axis runs over, the one named last changes fastest.
Arguments:
- latents: bfloat16 [2, 131072, 512], P('member', 'fsdp'), may hold values from -16 to 16
- noise: float32 [2, 32], P('member'), may hold values from -4 to 4
- cond_gain: float32 [32, 512], replicated, may hold values from -0.5 to 0.5
- cond_shift: float32 [32, 512], replicated, may hold values from -0.5 to 0.5
- w_in: bfloat16 [512, 2048], P('fsdp'), may hold values from -0.25 to 0.25
- b_in: float32 [2048], replicated, may hold values from -3 to 3
- w_out: bfloat16 [2048, 512], P('fsdp'), may hold values from -0.125 to 0.125
- target: bfloat16 [131072, 512], P('fsdp'), may hold values from -6 to 6
Outputs:
- prediction: bfloat16 [2, 131072, 512], P('member', 'fsdp')
- grad_in: float32 [512, 2048], P('fsdp')
- grad_out: float32 [2048, 512], P('fsdp')
- crps_mean: float32 [], replicated
The draws below stay inside these ranges and needn't reach their ends.
All inputs are finite; a program needn't handle non-finite values.
Results may differ from the reference program's by a relative error of at most 0.0043.
Values may be sent and summed in bfloat16 or wider, within the bound.
A program may use at most 128 MiB of HBM per device.

```python
import jax
import jax.numpy as jnp
from jax import lax

D = 512
H = 2048
ZN = 32
ROWS = 2048
NODES = 131072


def with_spikes(entries, stream_key, source, target, shards_of, factor):
    owner, partner = [(jnp.arange(entries.shape[axis_at]) // (entries.shape[axis_at] // shards_of)).reshape([-1 if axis == axis_at else 1 for axis in range(entries.ndim)]) for axis_at in (source, target)]
    chosen = jax.random.permutation(stream_key, shards_of)[partner]
    strong = (owner == chosen) | (owner == (partner + shards_of // 2) % shards_of)
    return jnp.where(strong, factor * entries, entries)


def levels(key, extent, shards, smallest, top_value):
    def one(position, blocks):
        heights = jax.random.uniform(jax.random.fold_in(jax.random.fold_in(key, 6), position), (blocks,), jnp.float32, smallest / len(shards), top_value / len(shards))
        return jnp.repeat(jnp.exp(heights), extent[position] // blocks).reshape((-1,) + (1,) * (len(extent) - position - 1))

    factor_of = one(*shards[0])
    for cut in shards[1:]:
        factor_of = factor_of * one(*cut)
    return factor_of


def centred(stream_key, dims, scale, bound, pieces=(), kind=jnp.bfloat16):
    result = scale * jax.random.normal(stream_key, dims, jnp.float32)
    if pieces:
        result = result * levels(stream_key, dims, pieces, -0.22, 0.18)
    return jnp.clip(result, -bound, bound).astype(kind)


def heavy_noise(stream_key, extent, width, most, split, heavy, kind=jnp.bfloat16):
    array = width * jax.random.normal(stream_key, extent, jnp.float32)
    if split:
        array = array * levels(stream_key, extent, split, -0.22, 0.18)
    return jnp.clip(with_spikes(array, jax.random.fold_in(stream_key, 3), *heavy), -most, most).astype(kind)


def setup_inputs(seed: int = 0) -> dict:
    key_list = jax.random.split(jax.random.key(seed), 9)
    return {
        "latents": heavy_noise(key_list[0], (2, NODES, D), 1.0, 16.0, ((0, 2), (1, 64)), (1, 2, 64, 4.0)),
        "noise": centred(key_list[1], (2, ZN), 1.0, 4.0, ((0, 2),), jnp.float32),
        "cond_gain": centred(key_list[2], (ZN, D), (4 * ZN) ** -0.5, 0.5, (), jnp.float32),
        "cond_shift": centred(key_list[3], (ZN, D), (4 * ZN) ** -0.5, 0.5, (), jnp.float32),
        "w_in": centred(key_list[4], (D, H), D ** -0.5, 0.25, ((0, 64),)),
        "b_in": centred(key_list[5], (H,), 0.5, 3.0, (), jnp.float32),
        "w_out": centred(key_list[6], (H, D), H ** -0.5, 0.125, ((0, 64),)),
        "target": centred(key_list[7], (NODES, D), 1.0, 6.0, ((0, 64),)),
    }


COEF = 0.7978845608
CUBIC = 0.044715

def gelu_value(v):
    return 0.5 * v * (1.0 + jnp.tanh(COEF * (v + CUBIC * v * v * v)))

def gelu_slope(v):
    u = jnp.tanh(COEF * (v + CUBIC * v * v * v))
    return 0.5 * (1.0 + u) + 0.5 * v * (1.0 - u * u) * COEF * (1.0 + 3.0 * CUBIC * v * v)

def smooth(d):
    return jnp.sqrt(d * d + 0.0625)

def forward(block, noise_row, cond_gain, cond_shift, w_in, b_in):
    gain = 1.0 + jnp.dot(noise_row[None, :], cond_gain, precision=lax.Precision.HIGHEST, preferred_element_type=jnp.float32)[0]
    shift = jnp.dot(noise_row[None, :], cond_shift, precision=lax.Precision.HIGHEST, preferred_element_type=jnp.float32)[0]
    values = block.astype(jnp.float32)
    center = lax.optimization_barrier(jnp.mean(values, axis=1, keepdims=True))
    spread = lax.optimization_barrier(jnp.mean((values - center) ** 2, axis=1, keepdims=True))
    normed = ((values - center) / jnp.sqrt(spread + 0.25) * gain + shift).astype(jnp.bfloat16)
    pre = jnp.dot(normed, w_in, preferred_element_type=jnp.float32) + b_in
    act = gelu_value(pre).astype(jnp.bfloat16)
    return (normed, pre, act, values)

def reference(latents, noise, cond_gain, cond_shift, w_in, b_in, w_out, target):
    count = NODES // ROWS
    blocks = latents.reshape(2, count, ROWS, D)
    targets = target.reshape(count, ROWS, D)
    scale = 1.0 / jnp.sqrt(jnp.float32(2 * NODES))

    def predict(member):

        def one(block):
            normed, pre, act, values = forward(block, noise[member], cond_gain, cond_shift, w_in, b_in)
            return (values + jnp.dot(act, w_out, preferred_element_type=jnp.float32)).astype(jnp.bfloat16)
        return lax.map(one, blocks[member])
    preds = jnp.stack([predict(0), predict(1)])

    def accumulate(carry, items):
        grad_a, grad_b, total = carry
        first, second, tgt, pred_a, pred_b = items
        owns = [pred_a.astype(jnp.float32), pred_b.astype(jnp.float32)]
        tval = tgt.astype(jnp.float32)
        for member, block in ((0, first), (1, second)):
            normed, pre, act, values = forward(block, noise[member], cond_gain, cond_shift, w_in, b_in)
            mine = owns[member]
            other = owns[1 - member]
            near = mine - tval
            apart = mine - other
            total = total + jnp.sum(0.5 * smooth(near) - 0.25 * smooth(apart))
            dpred = ((0.5 * near / smooth(near) - 0.5 * apart / smooth(apart)) * scale).astype(jnp.bfloat16)
            dact = jnp.dot(dpred, w_out.T, preferred_element_type=jnp.float32)
            dpre = (dact * gelu_slope(pre)).astype(jnp.bfloat16)
            grad_a = grad_a + jnp.dot(normed.T, dpre, preferred_element_type=jnp.float32)
            grad_b = grad_b + jnp.dot(act.T, dpred, preferred_element_type=jnp.float32)
        return ((grad_a, grad_b, total), None)
    start = (jnp.zeros((D, H), jnp.float32), jnp.zeros((H, D), jnp.float32), jnp.zeros((), jnp.float32))
    (grad_in, grad_out, total), unused = lax.scan(accumulate, start, (blocks[0], blocks[1], targets, preds[0], preds[1]))
    crps_mean = total / jnp.float32(2 * NODES * D)
    return (preds.reshape(2, NODES, D), grad_in, grad_out, crps_mean)
```

```python
import jax
import jax.numpy as jnp
from jax import lax
from jax.experimental import pallas as pl
from jax.experimental.pallas import tpu as pltpu
from jax.sharding import Mesh
from jax.sharding import PartitionSpec as P

M, Z, Y, X, C = AXES = ("member", "fsdp_0", "fsdp_1", "fsdp_2", "fsdp_3")
FSDP = (Z, Y, X, C)
MESH = pl.DeviceIdType.MESH
F32 = jnp.float32
BF16 = jnp.bfloat16

COEF = 0.7978845608
CUBIC = 0.044715

D = 512
H = 2048
ROWS = 2048
HALF = 1024
NODES = 131072
TILE = 256
TILES = HALF // TILE


def remote(src, dst, send, recv, device):
    return pltpu.make_async_remote_copy(
        src_ref=src, dst_ref=dst, send_sem=send, recv_sem=recv, device_id=device, device_id_type=MESH
    )


def dot(a, b):
    return jnp.dot(a, b, preferred_element_type=F32)


def dot_t(a, b):
    return lax.dot_general(a, b, (((1,), (1,)), ((), ())), preferred_element_type=F32)


def gain_of(noise, cond):
    n = noise.shape[1]
    square = (n, n)
    same = lax.broadcasted_iota(jnp.int32, square, 0) == lax.broadcasted_iota(jnp.int32, square, 1)
    column = jnp.sum(jnp.where(same, jnp.broadcast_to(noise, square), 0.0), axis=1, keepdims=True)
    return jnp.sum(column * cond, axis=0, keepdims=True)


def kernel(
    latents, noise, cond_gain, cond_shift, w_in, b_in, w_out, target,
    out, g_in, g_out, loss,
    wi, wo, lat, tgt, pbuf, nrm, nt, dp, dt, act, slp, nz,
    si, so, ri, ro, ihr, ihq, ifr, ifq, ohr, ohq, ofr, ofq,
    ic, oc, jhr, jhq, jfr, jfq, phr, phq, pfr, pfq,
    xi, xir, xo, xor, yi, yir, yo, yor, cr, crr,
    s_ld, s_out, s_lat, r_lat, s_prd, r_prd, s_nz, r_nz,
    s_w0, r_w0, l_w0, s_ag, r_ag, s_sib, r_sib, s_core, r_core, s_rs, r_rs, s_x, r_x, s_cr, r_cr,
):
    m, z, y, h, c = [lax.axis_index(a) for a in AXES]
    up = {Y: {Y: lax.rem(y + 1, 4)}, Z: {Z: lax.rem(z + 1, 4)}}
    down = {Y: {Y: lax.rem(y + 3, 4)}, Z: {Z: lax.rem(z + 3, 4)}}
    place = {Y: y, Z: z}
    sib = {C: 1 - c}
    pair = {M: 1 - m}
    near = {X: 1 - h, M: 1 - m}
    cross = {X: 1 - h, M: 1 - m, C: 1 - c}

    mine, theirs = m * HALF, (1 - m) * HALF

    def load_own(t):
        return pltpu.make_async_copy(
            latents.at[0, pl.ds(mine + t * TILE, TILE)], lat.at[0, pl.ds(t * TILE, TILE)], s_ld.at[t]
        )

    load_target = pltpu.make_async_copy(target.at[pl.ds(mine, HALF)], tgt, s_ld.at[TILES])
    for t in range(TILES):
        load_own(t).start()
    load_target.start()

    barrier = pltpu.get_barrier_semaphore()
    greeted = [sib, pair, near, cross, up[Y], down[Y], up[Z], down[Z]]
    for other in greeted:
        pl.semaphore_signal(barrier, inc=1, device_id=other, device_id_type=MESH)
    pl.semaphore_wait(barrier, len(greeted))

    def shard_parts(h_from, c_from, c_to):
        row = 2 * h_from + c_from
        parts = []
        for k in range(2):
            col = pl.ds(pl.multiple_of(c_to * 1024 + k * 512, 512), 512)
            parts.append((w_in.at[:, col], wi.at[2 * c_to + k, z, y, pl.ds(8 * row, 8)]))
        for k in range(2):
            col = pl.ds(pl.multiple_of(c_to * 256 + k * 128, 128), 128)
            parts.append((w_out.at[:, col], wo.at[2 * c_to + k, z, y, pl.ds(32 * row, 32)]))
        return parts

    partners = [(near, 1 - h, c), (cross, 1 - h, 1 - c), (sib, h, 1 - c)]
    first_sends = []
    for n, (src, dst) in enumerate(shard_parts(h, c, c)):
        pltpu.make_async_copy(src, dst, l_w0.at[n]).start()
    for n in range(4):
        for r, (who, _, c_to) in enumerate(partners):
            src, dst = shard_parts(h, c, c_to)[n]
            copy = remote(src, dst, s_w0.at[r, n], r_w0.at[r, n], who)
            copy.start()
            first_sends.append(copy)

    noise_copy = remote(noise, nz, s_nz, r_nz, pair)
    noise_copy.start()

    def send_latents(t):
        return remote(
            latents.at[0, pl.ds(theirs + t * TILE, TILE)],
            lat.at[1, pl.ds(t * TILE, TILE)],
            s_lat.at[t],
            r_lat.at[t],
            pair,
        )

    for t in range(TILES):
        send_latents(t).start()

    streams = [(wi, 0, Y), (wi, 1, Z), (wo, 0, Y), (wo, 1, Z)]

    def other_axis(a):
        return Z if a == Y else Y

    def gather_view(s, phase, i, part):
        ref, k, first = streams[s]
        size = ref.shape[3]
        rows = pl.ds(0, size) if part is None else pl.ds(part * size // 2, size // 2)
        block = 2 * c + k
        if phase == 0:
            return ref.at[block, z, i, rows] if first == Y else ref.at[block, i, y, rows]
        return ref.at[block, i, :, rows] if first == Y else ref.at[block, :, i, rows]

    def gather_copy(s, phase, n):
        axis = streams[s][2] if phase == 0 else other_axis(streams[s][2])
        p = place[axis]
        i = [p, p, lax.rem(p + 3, 4), lax.rem(p + 1, 4)][n]
        view = gather_view(s, phase, i, [None, None, 0, 1][n])
        who = [up, down, up, down][n][axis]
        return remote(view, view, s_ag.at[s, phase, n], r_ag.at[s, phase, n], who)

    def gather_landed(s, phase, n):
        axis = streams[s][2] if phase == 0 else other_axis(streams[s][2])
        p = place[axis]
        i = lax.rem(p + [3, 1, 2, 2][n], 4)
        view = gather_view(s, phase, i, [None, None, 0, 1][n])
        remote(view, view, s_ag.at[s, phase, n], r_ag.at[s, phase, n], up[axis]).wait_recv()

    def gather_start(s, phase):
        gather_copy(s, phase, 0).start()
        gather_copy(s, phase, 1).start()

    def gather_forward(s, phase):
        gather_landed(s, phase, 0)
        gather_copy(s, phase, 2).start()
        gather_landed(s, phase, 1)
        gather_copy(s, phase, 3).start()

    def gather_end(s, phase):
        gather_landed(s, phase, 2)
        gather_landed(s, phase, 3)
        for n in range(4):
            gather_copy(s, phase, n).wait_send()

    def share(s, block_of):
        ref, k, _ = streams[s]
        view = ref.at[2 * block_of + k]
        return remote(view, view, s_sib.at[s], r_sib.at[s], sib)

    for n in range(4):
        src, dst = shard_parts(h, c, c)[n]
        pltpu.make_async_copy(src, dst, l_w0.at[n]).wait()
        for r, (who, h_from, c_from) in enumerate(partners):
            src, dst = shard_parts(h_from, c_from, c)[n]
            remote(src, dst, s_w0.at[r, n], r_w0.at[r, n], who).wait_recv()
        gather_start(n, 0)
    for copy in first_sends:
        copy.wait_send()
    for s in range(4):
        gather_forward(s, 0)
    for s in range(4):
        gather_end(s, 0)
        gather_start(s, 1)
    for s in range(4):
        gather_forward(s, 1)
    for s in range(4):
        gather_end(s, 1)
        share(s, c).start()

    noise_copy.wait()
    gains = [1.0 + gain_of(noise[...], cond_gain[...]), 1.0 + gain_of(nz[...], cond_gain[...])]
    shifts = [gain_of(noise[...], cond_shift[...]), gain_of(nz[...], cond_shift[...])]

    for s in range(4):
        share(s, c).wait_send()
        share(s, 1 - c).wait_recv()

    def w_out_rows(j):
        return jnp.concatenate([wo[b, j].reshape(512, 128) for b in range(4)], axis=1)

    def forward(slot, t):
        row = pl.multiple_of(slot * HALF + t * TILE, TILE)
        rows = pl.ds(row, TILE)
        x = lat[slot, pl.ds(pl.multiple_of(t * TILE, TILE), TILE), :].astype(F32)
        centred = x - jnp.mean(x, axis=1, keepdims=True)
        spread = jnp.mean(centred * centred, axis=1, keepdims=True)
        normed = centred * lax.rsqrt(spread + 0.25) * gains[slot] + shifts[slot]
        nrm[...] = normed.astype(BF16)
        nt[:, rows] = normed.T.astype(BF16)

        def hidden(j, carry):
            v = dot(nrm[...], wi[j].reshape(512, 512)) + b_in[pl.ds(j, 1), :]
            q = v * v
            u = jnp.tanh(v * (COEF + (COEF * CUBIC) * q))
            half = 0.5 + 0.5 * u
            a = v * half
            slope = half + a * ((1.0 - half) * (2.0 * COEF + (6.0 * COEF * CUBIC) * q))
            act[j, rows, :] = a.astype(BF16)
            slp[j, rows, :] = slope.astype(BF16)
            return carry

        lax.fori_loop(0, 4, hidden, 0)
        for j in range(4):
            x = x + dot(act[j, rows, :], w_out_rows(j))
        pbuf[slot, pl.ds(pl.multiple_of(t * TILE, TILE), TILE), :] = x.astype(BF16)

    def store_own(t):
        return pltpu.make_async_copy(
            pbuf.at[0, pl.ds(t * TILE, TILE)], out.at[0, pl.ds(mine + t * TILE, TILE)], s_out.at[t]
        )

    def send_prediction(t):
        return remote(
            pbuf.at[1, pl.ds(t * TILE, TILE)],
            out.at[0, pl.ds(mine + t * TILE, TILE)],
            s_prd.at[t],
            r_prd.at[t],
            pair,
        )

    def own_tile(t, carry):
        load_own(t).wait()
        forward(0, t)
        store_own(t).start()
        return carry

    lax.fori_loop(0, TILES, own_tile, 0)

    load_target.wait()
    cr[0] = jnp.zeros((8, 128), F32)
    scale = float((2 * NODES) ** -0.5)

    def both_tile(t, carry):
        send_latents(t).wait_recv()
        forward(1, t)
        send_prediction(t).start()
        rows = pl.ds(pl.multiple_of(t * TILE, TILE), TILE)
        p0 = pbuf[0, rows, :].astype(F32)
        p1 = pbuf[1, rows, :].astype(F32)
        goal = tgt[rows, :].astype(F32)
        near0, near1, apart = p0 - goal, p1 - goal, p0 - p1
        q0, q1, qa = near0 * near0 + 0.0625, near1 * near1 + 0.0625, apart * apart + 0.0625
        i0, i1, ia = lax.rsqrt(q0), lax.rsqrt(q1), lax.rsqrt(qa)
        crps = 0.5 * (q0 * i0 + q1 * i1 - qa * ia)
        summed = jnp.sum(crps.reshape(TILE // 8, 8, D), axis=0)
        cr[0] += sum(summed[:, k * 128 : (k + 1) * 128] for k in range(4))
        pull = 0.5 * apart * ia
        grads = ((0.5 * near0 * i0 - pull) * scale, (0.5 * near1 * i1 + pull) * scale)
        for slot in range(2):
            dp[slot] = grads[slot].astype(BF16)
            dt[:, pl.ds(pl.multiple_of(slot * HALF + t * TILE, TILE), TILE)] = grads[slot].T.astype(BF16)

        def hidden(j, carry):
            w = w_out_rows(j)
            for slot in range(2):
                at = pl.ds(pl.multiple_of(slot * HALF + t * TILE, TILE), TILE)
                slp[j, at, :] = (dot_t(dp[slot], w) * slp[j, at, :].astype(F32)).astype(BF16)
            return carry

        lax.fori_loop(0, 4, hidden, 0)
        return carry

    lax.fori_loop(0, TILES, both_tile, 0)

    def core_copy(n, j, half):
        if n == 0:
            k = 2 * j + half
            return remote(si.at[1 - c, k], ri.at[k], s_core.at[0, k], r_core.at[0, k], sib)
        ys = pl.ds(2 * half, 2)
        k = 2 * j + half
        return remote(so.at[1 - c, j, ys], ro.at[j, ys], s_core.at[1, k], r_core.at[1, k], sib)

    def grads_of(j, carry):
        for half in range(2):
            cols = slice(256 * half, 256 * half + 256)
            gi = dot(nt[...], slp[j, :, cols]).reshape(32, 2, 8, 256)
            go = dot(dt[...], act[j, :, cols]).T.reshape(2, 2, 2, 32, 512)
            for core in range(2):
                si[core, 2 * j + half] = gi[:, core].reshape(4, 4, 16, 256).astype(BF16)
                so[core, j, 2 * half : 2 * half + 2] = go[:, :, core].reshape(2, 64, 512).astype(BF16)
            core_copy(0, j, half).start()
            core_copy(1, j, half).start()
        return carry

    lax.fori_loop(0, 4, grads_of, 0)

    def add_sibling(j, carry):
        for half in range(2):
            k = 2 * j + half
            core_copy(0, j, half).wait()
            si[c, k] = (si[c, k].astype(F32) + ri[k].astype(F32)).astype(BF16)
            core_copy(1, j, half).wait()
            ys = pl.ds(2 * half, 2)
            so[c, j, ys] = (so[c, j, ys].astype(F32) + ro[j, ys].astype(F32)).astype(BF16)
        return carry

    lax.fori_loop(0, 4, add_sibling, 0)

    mates = [
        sib,
        near,
        pair,
        {Y: y + 1 - 2 * lax.rem(y, 2)},
        {Y: 3 - y},
        {Z: z + 1 - 2 * lax.rem(z, 2)},
        {Z: 3 - z},
    ]

    def loss_copy(n):
        return remote(cr.at[n], crr.at[n], s_cr.at[n], r_cr.at[n], mates[n])

    def loss_next(n):
        loss_copy(n).wait()
        cr[n + 1] = cr[n] + crr[n]
        if n + 1 < len(mates):
            loss_copy(n + 1).start()

    loss_copy(0).start()

    def i_first(i, part):
        return si.at[c, pl.ds(4 * part, 4), :, i]

    def o_first(i, part):
        return so.at[c, i, :, pl.ds(32 * part, 32)]

    def i_second(i, part):
        return ic.at[pl.ds(4 * part, 4), i]

    def o_second(i, part):
        return oc.at[i, pl.ds(32 * part, 32)]

    def ring_sums(n, axis, view, hr, hq, fr, fq):
        p = place[axis]
        q, r, o = lax.rem(p + 1, 4), lax.rem(p + 3, 4), lax.rem(p + 2, 4)

        def move(k):
            src, dst, who = [
                (view(o, 0), hr, up),
                (view(o, 1), hq, down),
                (view(q, 1), fr.at[1], up),
                (view(r, 0), fq.at[0], down),
                (view(q, 0), fr.at[0], up),
                (view(r, 1), fq.at[1], down),
            ][k]
            return remote(src, dst, s_rs.at[n, k], r_rs.at[n, k], who[axis])

        def begin():
            for k in range(4):
                move(k).start()

        def middle():
            for k, i, part, got in ((0, q, 0, hr), (1, r, 1, hq)):
                move(k).wait_recv()
                block = view(i, part)
                block[...] = (block[...].astype(F32) + got[...].astype(F32)).astype(BF16)
                move(4 + k).start()

        def end():
            for k in (2, 3, 4, 5):
                move(k).wait_recv()
            sums = []
            for part in range(2):
                sums.append(
                    view(p, part)[...].astype(F32) + (fr[part].astype(F32) + fq[part].astype(F32))
                )
            for k in range(6):
                move(k).wait_send()
            return sums

        return begin, middle, end

    i1 = ring_sums(0, Y, i_first, ihr, ihq, ifr, ifq)
    o1 = ring_sums(1, Z, o_first, ohr, ohq, ofr, ofq)
    i2 = ring_sums(2, Z, i_second, jhr, jhq, jfr, jfq)
    o2 = ring_sums(3, Y, o_second, phr, phq, pfr, pfq)
    i1[0]()
    o1[0]()
    loss_next(0)
    i1[1]()
    o1[1]()
    loss_next(1)
    for part, v in enumerate(i1[2]()):
        ic[4 * part : 4 * part + 4] = v.astype(BF16)
    i2[0]()
    for part, v in enumerate(o1[2]()):
        oc[:, 32 * part : 32 * part + 32] = v.astype(BF16)
    o2[0]()
    loss_next(2)
    i2[1]()
    o2[1]()
    loss_next(3)
    sum_i = jnp.concatenate(i2[2](), axis=0)
    xi[...] = jnp.where(h == 0, sum_i[:, 8:], sum_i[:, :8])
    i_copy = remote(xi, xir, s_x.at[0], r_x.at[0], near)
    i_copy.start()
    low, high = o2[2]()
    xo[...] = jnp.where(h == 0, high, low)
    o_copy = remote(xo, xor, s_x.at[1], r_x.at[1], near)
    o_copy.start()
    own_i = jnp.where(h == 0, sum_i[:, :8], sum_i[:, 8:])
    own_o = jnp.where(h == 0, low, high)
    loss_next(4)
    i_copy.wait()
    yi[...] = own_i + xir[...]
    i_copy = remote(yi, yir, s_x.at[2], r_x.at[2], pair)
    i_copy.start()
    o_copy.wait()
    yo[...] = own_o + xor[...]
    o_copy = remote(yo, yor, s_x.at[3], r_x.at[3], pair)
    o_copy.start()
    loss_next(5)
    i_copy.wait()
    for k in range(8):
        g_in[:, 256 * k : 256 * k + 256] = yi[k] + yir[k]
    o_copy.wait()
    g_out[...] = yo[...] + yor[...]
    loss_next(6)
    loss[0, 0] = jnp.sum(cr[7]) / float(2 * NODES * D)

    for t in range(TILES):
        store_own(t).wait()
        send_latents(t).wait_send()
        send_prediction(t).wait_send()
        remote(
            pbuf.at[1, pl.ds(t * TILE, TILE)],
            out.at[0, pl.ds(theirs + t * TILE, TILE)],
            s_prd.at[t],
            r_prd.at[t],
            pair,
        ).wait_recv()


def vm(*shape, dtype=BF16):
    return pltpu.VMEM(shape, dtype)


def dma(*shape):
    return pltpu.SemaphoreType.DMA(shape)


SCRATCH = [
    vm(4, 4, 4, 32, 512), vm(4, 4, 4, 128, 128), vm(2, HALF, D), vm(HALF, D), vm(2, HALF, D),
    vm(TILE, D), vm(D, ROWS), vm(2, TILE, D), vm(D, ROWS), vm(4, ROWS, 512), vm(4, ROWS, 512), vm(1, 32, dtype=F32),
    vm(2, 8, 4, 4, 16, 256), vm(2, 4, 4, 64, 512), vm(8, 4, 4, 16, 256), vm(4, 4, 64, 512),
    vm(4, 4, 16, 256), vm(4, 4, 16, 256), vm(2, 4, 4, 16, 256), vm(2, 4, 4, 16, 256),
    vm(4, 32, 512), vm(4, 32, 512), vm(2, 4, 32, 512), vm(2, 4, 32, 512),
    vm(8, 4, 16, 256), vm(4, 64, 512),
    vm(4, 16, 256), vm(4, 16, 256), vm(2, 4, 16, 256), vm(2, 4, 16, 256),
    vm(32, 512), vm(32, 512), vm(2, 32, 512), vm(2, 32, 512),
    vm(8, 8, 256, dtype=F32), vm(8, 8, 256, dtype=F32), vm(32, 512, dtype=F32), vm(32, 512, dtype=F32),
    vm(8, 8, 256, dtype=F32), vm(8, 8, 256, dtype=F32), vm(32, 512, dtype=F32), vm(32, 512, dtype=F32),
    vm(8, 8, 128, dtype=F32), vm(7, 8, 128, dtype=F32),
    dma(TILES + 1), dma(TILES), dma(TILES), dma(TILES), dma(TILES), dma(TILES),
    pltpu.SemaphoreType.DMA, pltpu.SemaphoreType.DMA,
    dma(3, 4), dma(3, 4), dma(4), dma(4, 2, 4), dma(4, 2, 4), dma(4), dma(4), dma(2, 8), dma(2, 8),
    dma(4, 6), dma(4, 6), dma(4), dma(4), dma(7), dma(7),
]


def on_device(latents, noise, cond_gain, cond_shift, w_in, b_in, w_out, target):
    inside = pl.BlockSpec(memory_space=pltpu.VMEM)
    anywhere = pl.BlockSpec(memory_space=pl.ANY)
    prediction, grad_in, grad_out, loss = pl.pallas_call(
        kernel,
        out_shape=(
            jax.ShapeDtypeStruct((1, ROWS, D), BF16),
            jax.ShapeDtypeStruct((8, H), F32),
            jax.ShapeDtypeStruct((32, D), F32),
            jax.ShapeDtypeStruct((1, 1), F32),
        ),
        in_specs=[anywhere] + [inside] * 6 + [anywhere],
        out_specs=(anywhere, inside, inside, pl.BlockSpec(memory_space=pltpu.SMEM)),
        scratch_shapes=SCRATCH,
        compiler_params=pltpu.CompilerParams(
            collective_id=0, has_side_effects=True, vmem_limit_bytes=63 * 1024 * 1024
        ),
    )(latents, noise, cond_gain, cond_shift, w_in, b_in.reshape(4, 512), w_out, target)
    return prediction, grad_in, grad_out, loss.reshape(())


def solution(mesh):
    torus = Mesh(mesh.devices.reshape(2, 4, 4, 2, 2), AXES)
    in_specs = (
        P(M, FSDP, None),
        P(M, None),
        P(),
        P(),
        P(FSDP, None),
        P(),
        P(FSDP, None),
        P(FSDP, None),
    )
    out_specs = (P(M, FSDP, None), P(FSDP, None), P(FSDP, None), P())
    return jax.shard_map(on_device, mesh=torus, in_specs=in_specs, out_specs=out_specs, check_vma=False)
```

```python
import functools

import jax
import jax.numpy as jnp
from jax import lax
from jax.experimental import pallas as pl
from jax.experimental.pallas import tpu as pltpu
from jax.sharding import Mesh
from jax.sharding import PartitionSpec as P

M, Z, Y, X, C = AXES = ("member", "fsdp_0", "fsdp_1", "fsdp_2", "fsdp_3")
FSDP = (Z, Y, X, C)
MESH = pl.DeviceIdType.MESH
F32 = jnp.float32
BF16 = jnp.bfloat16

COEF = 0.7978845608
CUBIC = 0.044715

D = 512
H = 2048
ROWS = 2048
HALF = 1024
NODES = 131072
TILE = 256
TILES = HALF // TILE


def remote(src, dst, send, recv, device):
    return pltpu.make_async_remote_copy(
        src_ref=src, dst_ref=dst, send_sem=send, recv_sem=recv, device_id=device, device_id_type=MESH
    )


def dot(a, b):
    return jnp.dot(a, b, preferred_element_type=F32)


def dot_t(a, b):
    return lax.dot_general(a, b, (((1,), (1,)), ((), ())), preferred_element_type=F32)


def gain_of(noise, cond):
    n = noise.shape[1]
    square = (n, n)
    same = lax.broadcasted_iota(jnp.int32, square, 0) == lax.broadcasted_iota(jnp.int32, square, 1)
    column = jnp.sum(jnp.where(same, jnp.broadcast_to(noise, square), 0.0), axis=1, keepdims=True)
    return jnp.sum(column * cond, axis=0, keepdims=True)


def kernel(
    latents, noise, cond_gain, cond_shift, w_in, b_in, w_out, target,
    out, g_in, g_out, loss,
    wi, wo, lat, tgt, pbuf, nrm, nt, dp, dt, act, slp, nz,
    si, so, ri, ro, ihr, ihq, ifr, ifq, ohr, ohq, ofr, ofq,
    ic, oc, jhr, jhq, jfr, jfq, phr, phq, pfr, pfq,
    xi, xir, xo, xor, cr, crr,
    s_ld, s_out, s_lat, r_lat, s_prd, r_prd, s_nz, r_nz,
    s_w0, r_w0, l_w0, s_ag, r_ag, s_sib, r_sib, s_core, r_core, s_rs, r_rs, s_x, r_x, s_cr, r_cr,
):
    m, z, y, h, c = [lax.axis_index(a) for a in AXES]
    up = {Y: {Y: lax.rem(y + 1, 4)}, Z: {Z: lax.rem(z + 1, 4)}}
    down = {Y: {Y: lax.rem(y + 3, 4)}, Z: {Z: lax.rem(z + 3, 4)}}
    place = {Y: y, Z: z}
    sib = {C: 1 - c}
    pair = {M: 1 - m}
    near = {X: 1 - h, M: 1 - m}
    cross = {X: 1 - h, M: 1 - m, C: 1 - c}

    mine, theirs = m * HALF, (1 - m) * HALF

    def load_own(t):
        return pltpu.make_async_copy(
            latents.at[0, pl.ds(mine + t * TILE, TILE)], lat.at[0, pl.ds(t * TILE, TILE)], s_ld.at[t]
        )

    load_target = pltpu.make_async_copy(target.at[pl.ds(mine, HALF)], tgt, s_ld.at[TILES])
    for t in range(TILES):
        load_own(t).start()
    load_target.start()

    barrier = pltpu.get_barrier_semaphore()
    greeted = [sib, pair, near, cross, {X: 1 - h}, up[Y], down[Y], up[Z], down[Z]]
    for other in greeted:
        pl.semaphore_signal(barrier, inc=1, device_id=other, device_id_type=MESH)
    pl.semaphore_wait(barrier, len(greeted))

    def shard_parts(h_from, c_from, c_to):
        row = 2 * h_from + c_from
        parts = []
        for k in range(2):
            col = pl.ds(pl.multiple_of(c_to * 1024 + k * 512, 512), 512)
            parts.append((w_in.at[:, col], wi.at[2 * c_to + k, z, y, pl.ds(8 * row, 8)]))
        for k in range(2):
            col = pl.ds(pl.multiple_of(c_to * 256 + k * 128, 128), 128)
            parts.append((w_out.at[:, col], wo.at[2 * c_to + k, z, y, pl.ds(32 * row, 32)]))
        return parts

    partners = [(near, 1 - h, c), (cross, 1 - h, 1 - c), (sib, h, 1 - c)]
    first_sends = []
    for n, (src, dst) in enumerate(shard_parts(h, c, c)):
        pltpu.make_async_copy(src, dst, l_w0.at[n]).start()
    for n in range(4):
        for r, (who, _, c_to) in enumerate(partners):
            src, dst = shard_parts(h, c, c_to)[n]
            copy = remote(src, dst, s_w0.at[r, n], r_w0.at[r, n], who)
            copy.start()
            first_sends.append(copy)

    noise_copy = remote(noise, nz, s_nz, r_nz, pair)
    noise_copy.start()

    def send_latents(t):
        return remote(
            latents.at[0, pl.ds(theirs + t * TILE, TILE)],
            lat.at[1, pl.ds(t * TILE, TILE)],
            s_lat.at[t],
            r_lat.at[t],
            pair,
        )

    for t in range(TILES):
        send_latents(t).start()

    def tile_of(slot, t):
        return pl.ds(pl.multiple_of(slot * HALF + t * TILE, TILE), TILE)

    def normalise(slot, t, gain, shift):
        if slot == 0:
            load_own(t).wait()
        else:
            send_latents(t).wait_recv()
        x = lat[slot, tile_of(0, t), :].astype(F32)
        centred = x - jnp.mean(x, axis=1, keepdims=True)
        spread = jnp.mean(centred * centred, axis=1, keepdims=True)
        normed = centred * lax.rsqrt(spread + 0.25) * gain + shift
        nt[:, tile_of(slot, t)] = normed.T.astype(BF16)
        nrm[slot, tile_of(0, t), :] = normed.astype(BF16)

    gain, shift = 1.0 + gain_of(noise[...], cond_gain[...]), gain_of(noise[...], cond_shift[...])
    for t in range(2):
        normalise(0, t, gain, shift)
    streams = [(wi, 0, Y), (wi, 1, Z), (wo, 0, Y), (wo, 1, Z)]

    def other_axis(a):
        return Z if a == Y else Y

    def gather_view(s, phase, i, part):
        ref, k, first = streams[s]
        size = ref.shape[3]
        rows = pl.ds(0, size) if part is None else pl.ds(part * size // 2, size // 2)
        block = 2 * c + k
        if phase == 0:
            return ref.at[block, z, i, rows] if first == Y else ref.at[block, i, y, rows]
        return ref.at[block, i, :, rows] if first == Y else ref.at[block, :, i, rows]

    def gather_copy(s, phase, n):
        axis = streams[s][2] if phase == 0 else other_axis(streams[s][2])
        p = place[axis]
        i = [p, p, lax.rem(p + 3, 4), lax.rem(p + 1, 4)][n]
        view = gather_view(s, phase, i, [None, None, 0, 1][n])
        who = [up, down, up, down][n][axis]
        return remote(view, view, s_ag.at[s, phase, n], r_ag.at[s, phase, n], who)

    def gather_landed(s, phase, n):
        axis = streams[s][2] if phase == 0 else other_axis(streams[s][2])
        p = place[axis]
        i = lax.rem(p + [3, 1, 2, 2][n], 4)
        view = gather_view(s, phase, i, [None, None, 0, 1][n])
        remote(view, view, s_ag.at[s, phase, n], r_ag.at[s, phase, n], up[axis]).wait_recv()

    def gather_start(s, phase):
        gather_copy(s, phase, 0).start()
        gather_copy(s, phase, 1).start()

    def gather_forward(s, phase):
        gather_landed(s, phase, 0)
        gather_copy(s, phase, 2).start()
        gather_landed(s, phase, 1)
        gather_copy(s, phase, 3).start()

    def gather_end(s, phase):
        gather_landed(s, phase, 2)
        gather_landed(s, phase, 3)
        for n in range(4):
            gather_copy(s, phase, n).wait_send()

    def share(s, block_of):
        ref, k, _ = streams[s]
        view = ref.at[2 * block_of + k]
        return remote(view, view, s_sib.at[s], r_sib.at[s], sib)

    for n in range(4):
        src, dst = shard_parts(h, c, c)[n]
        pltpu.make_async_copy(src, dst, l_w0.at[n]).wait()
        for r, (who, h_from, c_from) in enumerate(partners):
            src, dst = shard_parts(h_from, c_from, c)[n]
            remote(src, dst, s_w0.at[r, n], r_w0.at[r, n], who).wait_recv()
        gather_start(n, 0)
    normalise(0, 2, gain, shift)
    for s in range(4):
        gather_forward(s, 0)
    normalise(0, 3, gain, shift)
    for s in range(2):
        gather_end(s, 0)
        gather_start(s, 1)
    noise_copy.wait()
    other_gain, other_shift = 1.0 + gain_of(nz[...], cond_gain[...]), gain_of(nz[...], cond_shift[...])
    normalise(1, 0, other_gain, other_shift)
    for s in range(2):
        gather_forward(s, 1)
    for s in range(2, 4):
        gather_end(s, 0)
        gather_start(s, 1)
    normalise(1, 1, other_gain, other_shift)
    for s in range(2):
        gather_end(s, 1)
        share(s, c).start()
    for s in range(2):
        share(s, 1 - c).wait_recv()

    def w_out_rows(j):
        return jnp.concatenate([wo[b, j].reshape(512, 128) for b in range(4)], axis=1)

    def hidden(j, slot, t):
        rows = tile_of(slot, t)
        v = dot(nrm[slot, tile_of(0, t), :], wi[j].reshape(512, 512)) + b_in[:, 512 * j : 512 * j + 512]
        q = v * v
        u = jnp.tanh(v * (COEF + (COEF * CUBIC) * q))
        half = 0.5 + 0.5 * u
        a = v * half
        slope = half + a * ((1.0 - half) * (2.0 * COEF + (6.0 * COEF * CUBIC) * q))
        a = a.astype(BF16)
        act[j, rows, :] = a
        slp[j, rows, :] = slope.astype(BF16)
        return a

    def store_own(t):
        return pltpu.make_async_copy(
            pbuf.at[0, pl.ds(t * TILE, TILE)], out.at[0, pl.ds(mine + t * TILE, TILE)], s_out.at[t]
        )

    def send_prediction(t):
        return remote(
            pbuf.at[1, pl.ds(t * TILE, TILE)],
            out.at[0, pl.ds(mine + t * TILE, TILE)],
            s_prd.at[t],
            r_prd.at[t],
            pair,
        )

    def own_hidden(t, carry):
        for j in range(4):
            hidden(j, 0, t)
        return carry

    def partner_hidden(t, carry):
        for j in range(4):
            hidden(j, 1, t)
        return carry

    def own_out(t, carry):
        x = lat[0, tile_of(0, t), :].astype(F32)
        for j in range(4):
            x = x + dot(act[j, tile_of(0, t), :], w_out_rows(j))
        pbuf[0, tile_of(0, t), :] = x.astype(BF16)
        store_own(t).start()
        return carry

    lax.fori_loop(0, 2, own_hidden, 0)
    for s in range(2, 4):
        gather_forward(s, 1)
    normalise(1, 2, other_gain, other_shift)
    lax.fori_loop(2, TILES, own_hidden, 0)
    normalise(1, 3, other_gain, other_shift)
    lax.fori_loop(0, 2, partner_hidden, 0)
    for s in range(2, 4):
        gather_end(s, 1)
        share(s, c).start()
    for s in range(2, 4):
        share(s, 1 - c).wait_recv()
    lax.fori_loop(0, TILES, own_out, 0)

    load_target.wait()
    cr[0] = jnp.zeros((8, 128), F32)
    scale = float((2 * NODES) ** -0.5)

    def both_tile(ready, t, carry):
        x = lat[1, tile_of(0, t), :].astype(F32)
        for j in range(4):
            a = act[j, tile_of(1, t), :] if ready else hidden(j, 1, t)
            x = x + dot(a, w_out_rows(j))
        pbuf[1, tile_of(0, t), :] = x.astype(BF16)
        send_prediction(t).start()
        rows = tile_of(0, t)
        p0 = pbuf[0, rows, :].astype(F32)
        p1 = x.astype(BF16).astype(F32)
        goal = tgt[rows, :].astype(F32)
        near0, near1, apart = p0 - goal, p1 - goal, p0 - p1
        q0, q1, qa = near0 * near0 + 0.0625, near1 * near1 + 0.0625, apart * apart + 0.0625
        i0, i1, ia = lax.rsqrt(q0), lax.rsqrt(q1), lax.rsqrt(qa)
        crps = q0 * i0 + q1 * i1 - qa * ia
        summed = jnp.sum(crps.reshape(TILE // 8, 8, D), axis=0)
        cr[0] += sum(summed[:, k * 128 : (k + 1) * 128] for k in range(4))
        pull = (0.5 * scale) * (apart * ia)
        grads = ((0.5 * scale) * (near0 * i0) - pull, (0.5 * scale) * (near1 * i1) + pull)
        for slot in range(2):
            dp[slot] = grads[slot].astype(BF16)
            dt[:, tile_of(slot, t)] = grads[slot].T.astype(BF16)
        for j in range(4):
            w = w_out_rows(j)
            for slot in range(2):
                at = tile_of(slot, t)
                slp[j, at, :] = (dot_t(dp[slot], w) * slp[j, at, :].astype(F32)).astype(BF16)
        return carry

    lax.fori_loop(0, 2, functools.partial(both_tile, True), 0)
    lax.fori_loop(2, TILES, functools.partial(both_tile, False), 0)

    mates = [
        sib,
        near,
        pair,
        {Y: y + 1 - 2 * lax.rem(y, 2)},
        {Y: 3 - y},
        {Z: z + 1 - 2 * lax.rem(z, 2)},
        {Z: 3 - z},
    ]

    def loss_copy(n):
        return remote(cr.at[n], crr.at[n], s_cr.at[n], r_cr.at[n], mates[n])

    def loss_next(n):
        loss_copy(n).wait()
        cr[n + 1] = cr[n] + crr[n]
        if n + 1 < len(mates):
            loss_copy(n + 1).start()

    blocks = [lax.rem(z + 2, 4), lax.rem(z + 1, 4), lax.rem(z + 3, 4), z]

    def core_copy(n, s, half):
        j, k = blocks[s], 2 * s + half
        if n == 0:
            at = 2 * j + half
            return remote(si.at[1 - c, at], ri.at[at], s_core.at[0, k], r_core.at[0, k], sib)
        ys = pl.ds(2 * half, 2)
        return remote(so.at[1 - c, j, ys], ro.at[j, ys], s_core.at[1, k], r_core.at[1, k], sib)

    def i_block(s):
        j = blocks[s]
        gi = dot(nt[...], slp[j]).reshape(32, 2, 8, 512)
        for half in range(2):
            for core in range(2):
                part = gi[:, core, :, 256 * half : 256 * half + 256]
                si[core, 2 * j + half] = part.reshape(4, 4, 16, 256).astype(BF16)
        for half in range(2):
            core_copy(0, s, half).start()

    def o_block(s):
        j = blocks[s]
        go = dot(dt[...], act[j]).T.reshape(4, 2, 2, 32, 512)
        for core in range(2):
            so[core, j] = go[:, :, core].reshape(4, 64, 512).astype(BF16)
        for half in range(2):
            core_copy(1, s, half).start()

    def i_add(s):
        for half in range(2):
            core_copy(0, s, half).wait_recv()
            k = 2 * blocks[s] + half
            si[c, k] = (si[c, k].astype(F32) + ri[k].astype(F32)).astype(BF16)

    def o_add(s):
        j = blocks[s]
        for half in range(2):
            core_copy(1, s, half).wait_recv()
            ys = pl.ds(2 * half, 2)
            so[c, j, ys] = (so[c, j, ys].astype(F32) + ro[j, ys].astype(F32)).astype(BF16)

    class Ring:
        def __init__(self, n, axis, view, hr, hq, fr, fq):
            p = place[axis]
            q, r, o = lax.rem(p + 1, 4), lax.rem(p + 3, 4), lax.rem(p + 2, 4)
            self.n, self.axis, self.view, self.p, self.q, self.r = n, axis, view, p, q, r
            self.hr, self.hq, self.fr, self.fq = hr, hq, fr, fq
            self.moves = [
                (view(o, 0), hr, up),
                (view(o, 1), hq, down),
                (view(q, 1), fr.at[1], up),
                (view(r, 0), fq.at[0], down),
                (view(q, 0), fr.at[0], up),
                (view(r, 1), fq.at[1], down),
            ]

        def move(self, k):
            src, dst, who = self.moves[k]
            return remote(src, dst, s_rs.at[self.n, k], r_rs.at[self.n, k], who[self.axis])

        def start(self, *ks):
            for k in ks:
                self.move(k).start()

        def relay(self, k):
            i, part, got = [(self.q, 0, self.hr), (self.r, 1, self.hq)][k]
            self.move(k).wait_recv()
            block = self.view(i, part)
            block[...] = (block[...].astype(F32) + got[...].astype(F32)).astype(BF16)
            self.move(4 + k).start()

        def begin(self):
            self.start(0, 1, 2, 3)

        def middle(self):
            self.relay(0)
            self.relay(1)

        def end(self):
            for k in (2, 3, 4, 5):
                self.move(k).wait_recv()
            return [
                self.view(self.p, part)[...].astype(F32)
                + (self.fr[part].astype(F32) + self.fq[part].astype(F32))
                for part in range(2)
            ]

        def drain(self):
            for k in range(6):
                self.move(k).wait_send()

    def i_ring(s):
        return Ring(
            s, Y, lambda i, part: si.at[c, 2 * blocks[s] + part, :, i],
            ihr.at[s], ihq.at[s], ifr.at[s], ifq.at[s],
        )

    i1 = [i_ring(s) for s in range(4)]
    i2 = Ring(4, Z, lambda i, part: ic.at[pl.ds(4 * part, 4), i], jhr, jhq, jfr, jfq)
    o1 = Ring(5, Z, lambda i, part: so.at[c, i, :, pl.ds(32 * part, 32)], ohr, ohq, ofr, ofq)
    o2 = Ring(6, Y, lambda i, part: oc.at[i, pl.ds(32 * part, 32)], phr, phq, pfr, pfq)

    def i_end(s):
        for part, v in enumerate(i1[s].end()):
            ic[2 * blocks[s] + part] = v.astype(BF16)

    far = {X: 1 - h}

    def x_copies(n, send, got):
        ends = [(near, 1 - h), (far, 1 - h), (pair, h)]
        return [
            remote(send.at[part], got.at[k], s_x.at[n, k], r_x.at[n, k], who)
            for k, (who, part) in enumerate(ends)
        ]

    x_i, x_o = x_copies(0, xi, xir), x_copies(1, xo, xor)

    def x_sum(copies, send, got):
        for copy in copies:
            copy.wait_recv()
        own, beside, across, mate = [v.astype(F32) for v in (send[h], got[0], got[1], got[2])]
        return (own + beside) + (mate + across)

    loss_copy(0).start()
    i_block(0)
    o_block(0)
    i_add(0)
    i1[0].begin()
    i_block(1)
    o_add(0)
    o1.start(0, 1)
    loss_next(0)
    o_block(1)
    i_add(1)
    i1[1].begin()
    i_block(2)
    o_add(1)
    o1.start(2)
    i1[0].middle()
    loss_next(1)
    i_block(3)
    i_add(2)
    i1[2].begin()
    o_block(2)
    i_add(3)
    i1[3].begin()
    i1[1].middle()
    o1.relay(0)
    loss_next(2)
    o_block(3)
    o_add(2)
    o1.start(3)
    o1.relay(1)
    i1[2].middle()
    i_end(0)
    o_add(3)
    i1[3].middle()
    i_end(1)
    loss_next(3)
    i_end(2)
    i_end(3)
    i2.begin()
    for part, v in enumerate(o1.end()):
        oc[:, 32 * part : 32 * part + 32] = v.astype(BF16)
    o2.begin()
    loss_next(4)
    i2.middle()
    o2.middle()
    loss_next(5)
    sums = i2.end()
    for half in range(2):
        for part in range(2):
            xi[half, 4 * part : 4 * part + 4] = sums[part][:, 8 * half : 8 * half + 8].astype(BF16)
    for copy in x_i:
        copy.start()
    for part, v in enumerate(o2.end()):
        xo[part] = v.astype(BF16)
    for copy in x_o:
        copy.start()
    loss_next(6)
    loss[0, 0] = jnp.sum(cr[7]) * (0.5 / float(2 * NODES * D))
    total = x_sum(x_i, xi, xir)
    for k in range(8):
        g_in[:, 256 * k : 256 * k + 256] = total[k]
    g_out[...] = x_sum(x_o, xo, xor)

    for copy in first_sends + x_i + x_o:
        copy.wait_send()
    for s in range(4):
        share(s, c).wait_send()
        for n in range(2):
            for half in range(2):
                core_copy(n, s, half).wait_send()
    for ring in i1 + [i2, o1, o2]:
        ring.drain()
    for t in range(TILES):
        store_own(t).wait()
        send_latents(t).wait_send()
        send_prediction(t).wait_send()
        remote(
            pbuf.at[1, pl.ds(t * TILE, TILE)],
            out.at[0, pl.ds(theirs + t * TILE, TILE)],
            s_prd.at[t],
            r_prd.at[t],
            pair,
        ).wait_recv()


def finish(p_in, gi_in, go_in, p_out, gi_out, go_out, held, s_in, s_out):
    def step(n, k):
        part = pl.ds(256 * k, 256)
        if n == 0:
            return pltpu.make_async_copy(p_in.at[0, part], held.at[part], s_in.at[k])
        return pltpu.make_async_copy(held.at[part], p_out.at[0, part], s_out.at[k])

    for k in range(8):
        step(0, k).start()
    gi_out[...] = gi_in[...]
    go_out[...] = go_in[...]
    for k in range(8):
        step(0, k).wait()
        step(1, k).start()
    for k in range(8):
        step(1, k).wait()


def vm(*shape, dtype=BF16):
    return pltpu.VMEM(shape, dtype)


def dma(*shape):
    return pltpu.SemaphoreType.DMA(shape)


SCRATCH = [
    vm(4, 4, 4, 32, 512), vm(4, 4, 4, 128, 128), vm(2, HALF, D), vm(HALF, D), vm(2, HALF, D),
    vm(2, HALF, D), vm(D, ROWS), vm(2, TILE, D), vm(D, ROWS), vm(4, ROWS, 512), vm(4, ROWS, 512), vm(1, 32, dtype=F32),
    vm(2, 8, 4, 4, 16, 256), vm(2, 4, 4, 64, 512), vm(8, 4, 4, 16, 256), vm(4, 4, 64, 512),
    vm(4, 4, 16, 256), vm(4, 4, 16, 256), vm(4, 2, 4, 16, 256), vm(4, 2, 4, 16, 256),
    vm(4, 32, 512), vm(4, 32, 512), vm(2, 4, 32, 512), vm(2, 4, 32, 512),
    vm(8, 4, 16, 256), vm(4, 64, 512),
    vm(4, 16, 256), vm(4, 16, 256), vm(2, 4, 16, 256), vm(2, 4, 16, 256),
    vm(32, 512), vm(32, 512), vm(2, 32, 512), vm(2, 32, 512),
    vm(2, 8, 8, 256), vm(3, 8, 8, 256), vm(2, 32, 512), vm(3, 32, 512),
    vm(8, 8, 128, dtype=F32), vm(7, 8, 128, dtype=F32),
    dma(TILES + 1), dma(TILES), dma(TILES), dma(TILES), dma(TILES), dma(TILES),
    pltpu.SemaphoreType.DMA, pltpu.SemaphoreType.DMA,
    dma(3, 4), dma(3, 4), dma(4), dma(4, 2, 4), dma(4, 2, 4), dma(4), dma(4), dma(2, 8), dma(2, 8),
    dma(7, 6), dma(7, 6), dma(2, 3), dma(2, 3), dma(7), dma(7),
]


def on_device(latents, noise, cond_gain, cond_shift, w_in, b_in, w_out, target):
    inside = pl.BlockSpec(memory_space=pltpu.VMEM)
    anywhere = pl.BlockSpec(memory_space=pl.ANY)
    prediction, grad_in, grad_out, loss = pl.pallas_call(
        kernel,
        out_shape=(
            jax.ShapeDtypeStruct((1, ROWS, D), BF16),
            jax.ShapeDtypeStruct((8, H), F32),
            jax.ShapeDtypeStruct((32, D), F32),
            jax.ShapeDtypeStruct((1, 1), F32),
        ),
        in_specs=[anywhere] + [inside] * 6 + [anywhere],
        out_specs=(anywhere, inside, inside, pl.BlockSpec(memory_space=pltpu.SMEM)),
        scratch_shapes=SCRATCH,
        compiler_params=pltpu.CompilerParams(
            collective_id=0, has_side_effects=True, vmem_limit_bytes=63 * 1024 * 1024
        ),
    )(latents, noise, cond_gain, cond_shift, w_in, b_in.reshape(1, H), w_out, target)
    prediction, grad_in, grad_out = pl.pallas_call(
        finish,
        out_shape=(
            jax.ShapeDtypeStruct((1, ROWS, D), BF16),
            jax.ShapeDtypeStruct((8, H), F32),
            jax.ShapeDtypeStruct((32, D), F32),
        ),
        in_specs=[anywhere, inside, inside],
        out_specs=(anywhere, inside, inside),
        scratch_shapes=[vm(ROWS, D), dma(8), dma(8)],
    )(prediction, grad_in, grad_out)
    return prediction, grad_in, grad_out, loss.reshape(())


def solution(mesh):
    torus = Mesh(mesh.devices.reshape(2, 4, 4, 2, 2), AXES)
    in_specs = (
        P(M, FSDP, None),
        P(M, None),
        P(),
        P(),
        P(FSDP, None),
        P(),
        P(FSDP, None),
        P(FSDP, None),
    )
    out_specs = (P(M, FSDP, None), P(FSDP, None), P(FSDP, None), P())
    return jax.shard_map(on_device, mesh=torus, in_specs=in_specs, out_specs=out_specs, check_vma=False)
```

```python
import jax
import jax.numpy as jnp
from jax import lax
from jax.experimental import pallas as pl
from jax.experimental.pallas import tpu as pltpu
from jax.sharding import Mesh
from jax.sharding import PartitionSpec as P

M, Z, Y, X, C = AXES = ("member", "fsdp_0", "fsdp_1", "fsdp_2", "fsdp_3")
FSDP = (Z, Y, X, C)
MESH = pl.DeviceIdType.MESH
F32 = jnp.float32
BF16 = jnp.bfloat16

COEF = 0.7978845608
CUBIC = 0.044715

D = 512
H = 2048
ROWS = 2048
HALF = 1024
NODES = 131072
TILE = 256
TILES = HALF // TILE


def remote(src, dst, send, recv, device):
    return pltpu.make_async_remote_copy(
        src_ref=src, dst_ref=dst, send_sem=send, recv_sem=recv, device_id=device, device_id_type=MESH
    )


def dot(a, b):
    return jnp.dot(a, b, preferred_element_type=F32)


def dot_t(a, b):
    return lax.dot_general(a, b, (((1,), (1,)), ((), ())), preferred_element_type=F32)


def gain_of(noise, cond):
    n = noise.shape[1]
    square = (n, n)
    same = lax.broadcasted_iota(jnp.int32, square, 0) == lax.broadcasted_iota(jnp.int32, square, 1)
    column = jnp.sum(jnp.where(same, jnp.broadcast_to(noise, square), 0.0), axis=1, keepdims=True)
    return jnp.sum(column * cond, axis=0, keepdims=True)


def kernel(
    latents, noise, cond_gain, cond_shift, w_in, b_in, w_out, target,
    out, g_in, g_out, loss,
    wi, wo, lat, tgt, pbuf, nrm, nt, dp0, dp1, dt, act, slp, nz,
    si, so, ri, ro, ihr, ihq, ifr, ifq, ohr, ohq, ofr, ofq,
    ic, oc, jhr, jhq, jfr, jfq, phr, phq, pfr, pfq,
    xi, xir, xo, xor, cr, crr,
    s_ld, s_out, s_lat, r_lat, s_prd, r_prd, s_nz, r_nz,
    s_w0, r_w0, l_w0, s_ag, r_ag, s_sib, r_sib, s_core, r_core, s_rs, r_rs, s_x, r_x, s_cr, r_cr,
):
    m, z, y, h, c = [lax.axis_index(a) for a in AXES]
    up = {Y: {Y: lax.rem(y + 1, 4)}, Z: {Z: lax.rem(z + 1, 4)}}
    down = {Y: {Y: lax.rem(y + 3, 4)}, Z: {Z: lax.rem(z + 3, 4)}}
    away = {Y: {Y: lax.rem(y + 2, 4)}, Z: {Z: lax.rem(z + 2, 4)}}
    place = {Y: y, Z: z}
    sib = {C: 1 - c}
    pair = {M: 1 - m}
    near = {X: 1 - h, M: 1 - m}
    cross = {X: 1 - h, M: 1 - m, C: 1 - c}

    mine, theirs = m * HALF, (1 - m) * HALF

    def load_own(t):
        return pltpu.make_async_copy(
            latents.at[0, pl.ds(mine + t * TILE, TILE)], lat.at[0, pl.ds(t * TILE, TILE)], s_ld.at[t]
        )

    load_target = pltpu.make_async_copy(target.at[pl.ds(mine, HALF)], tgt, s_ld.at[TILES])
    for t in range(TILES):
        load_own(t).start()
    load_target.start()

    barrier = pltpu.get_barrier_semaphore()
    greeted = [sib, pair, near, cross, {X: 1 - h}, away[Y], away[Z], up[Y], down[Y], up[Z], down[Z]]
    for other in greeted:
        pl.semaphore_signal(barrier, inc=1, device_id=other, device_id_type=MESH)
    pl.semaphore_wait(barrier, len(greeted))

    def shard_parts(h_from, c_from, c_to):
        row = 2 * h_from + c_from
        parts = []
        for k in range(2):
            col = pl.ds(pl.multiple_of(c_to * 1024 + k * 512, 512), 512)
            parts.append((w_in.at[:, col], wi.at[2 * c_to + k, z, y, pl.ds(8 * row, 8)]))
        for k in range(2):
            col = pl.ds(pl.multiple_of(c_to * 256 + k * 128, 128), 128)
            parts.append((w_out.at[:, col], wo.at[2 * c_to + k, z, y, pl.ds(32 * row, 32)]))
        return parts

    partners = [(near, 1 - h, c), (cross, 1 - h, 1 - c), (sib, h, 1 - c)]
    first_sends = []
    for n, (src, dst) in enumerate(shard_parts(h, c, c)):
        pltpu.make_async_copy(src, dst, l_w0.at[n]).start()
    for n in range(4):
        for r, (who, _, c_to) in enumerate(partners):
            src, dst = shard_parts(h, c, c_to)[n]
            copy = remote(src, dst, s_w0.at[r, n], r_w0.at[r, n], who)
            copy.start()
            first_sends.append(copy)

    noise_copy = remote(noise, nz, s_nz, r_nz, pair)
    noise_copy.start()

    def send_latents(t):
        return remote(
            latents.at[0, pl.ds(theirs + t * TILE, TILE)],
            lat.at[1, pl.ds(t * TILE, TILE)],
            s_lat.at[t],
            r_lat.at[t],
            pair,
        )

    for t in range(TILES):
        send_latents(t).start()

    def tile_of(slot, t):
        return pl.ds(pl.multiple_of(slot * HALF + t * TILE, TILE), TILE)

    def normalise(slot, t, gain, shift):
        if slot == 0:
            load_own(t).wait()
        else:
            send_latents(t).wait_recv()
        x = lat[slot, tile_of(0, t), :].astype(F32)
        centred = x - jnp.mean(x, axis=1, keepdims=True)
        spread = jnp.mean(centred * centred, axis=1, keepdims=True)
        normed = centred * lax.rsqrt(spread + 0.25) * gain + shift
        nt[:, tile_of(slot, t)] = normed.T.astype(BF16)
        nrm[slot, tile_of(0, t), :] = normed.astype(BF16)

    gain, shift = 1.0 + gain_of(noise[...], cond_gain[...]), gain_of(noise[...], cond_shift[...])
    for t in range(2):
        normalise(0, t, gain, shift)
    streams = [(wi, 0, Y), (wi, 1, Z), (wo, 0, Y), (wo, 1, Z)]

    def other_axis(a):
        return Z if a == Y else Y

    def gather_view(s, phase, i, part):
        ref, k, first = streams[s]
        size = ref.shape[3]
        rows = pl.ds(0, size) if part is None else pl.ds(part * size // 2, size // 2)
        block = 2 * c + k
        if phase == 0:
            return ref.at[block, z, i, rows] if first == Y else ref.at[block, i, y, rows]
        return ref.at[block, i, :, rows] if first == Y else ref.at[block, :, i, rows]

    def gather_copy(s, phase, n):
        axis = streams[s][2] if phase == 0 else other_axis(streams[s][2])
        p = place[axis]
        if phase == 0:
            i, part, who = p, None, [up, down, away][n][axis]
        else:
            i = [p, p, lax.rem(p + 3, 4), lax.rem(p + 1, 4)][n]
            part, who = [None, None, 0, 1][n], [up, down, up, down][n][axis]
        view = gather_view(s, phase, i, part)
        return remote(view, view, s_ag.at[s, phase, n], r_ag.at[s, phase, n], who)

    def gather_landed(s, phase, n):
        axis = streams[s][2] if phase == 0 else other_axis(streams[s][2])
        p = place[axis]
        i = lax.rem(p + [3, 1, 2, 2][n], 4)
        view = gather_view(s, phase, i, None if phase == 0 else [None, None, 0, 1][n])
        remote(view, view, s_ag.at[s, phase, n], r_ag.at[s, phase, n], up[axis]).wait_recv()

    def gather_start(s, phase):
        for n in range(3 if phase == 0 else 2):
            gather_copy(s, phase, n).start()

    def gather_forward(s, phase):
        if phase == 0:
            return
        gather_landed(s, phase, 0)
        gather_copy(s, phase, 2).start()
        gather_landed(s, phase, 1)
        gather_copy(s, phase, 3).start()

    def gather_end(s, phase):
        for n in range(3) if phase == 0 else (2, 3):
            gather_landed(s, phase, n)

    def gather_drain(s, phase):
        for n in range(3 if phase == 0 else 4):
            gather_copy(s, phase, n).wait_send()

    def share(s, block_of):
        ref, k, _ = streams[s]
        view = ref.at[2 * block_of + k]
        return remote(view, view, s_sib.at[s], r_sib.at[s], sib)

    for n in range(4):
        src, dst = shard_parts(h, c, c)[n]
        pltpu.make_async_copy(src, dst, l_w0.at[n]).wait()
        for r, (who, h_from, c_from) in enumerate(partners):
            src, dst = shard_parts(h_from, c_from, c)[n]
            remote(src, dst, s_w0.at[r, n], r_w0.at[r, n], who).wait_recv()
        gather_start(n, 0)
    normalise(0, 2, gain, shift)
    for s in range(4):
        gather_forward(s, 0)
    normalise(0, 3, gain, shift)
    for s in range(2):
        gather_end(s, 0)
        gather_start(s, 1)
    noise_copy.wait()
    other_gain, other_shift = 1.0 + gain_of(nz[...], cond_gain[...]), gain_of(nz[...], cond_shift[...])
    normalise(1, 0, other_gain, other_shift)
    for s in range(2):
        gather_forward(s, 1)
    for s in range(2, 4):
        gather_end(s, 0)
        gather_start(s, 1)
    normalise(1, 1, other_gain, other_shift)
    for s in range(2):
        gather_end(s, 1)
        share(s, c).start()
    for s in range(2):
        share(s, 1 - c).wait_recv()

    def w_out_rows(j):
        return jnp.concatenate([wo[b, j].reshape(512, 128) for b in range(4)], axis=1)

    def hidden(j, slot, t):
        rows = tile_of(slot, t)
        v = dot(nrm[slot, tile_of(0, t), :], wi[j].reshape(512, 512)) + b_in[:, 512 * j : 512 * j + 512]
        q = v * v
        u = jnp.tanh(v * (COEF + (COEF * CUBIC) * q))
        half = 0.5 + 0.5 * u
        a = v * half
        slope = half + a * ((1.0 - half) * (2.0 * COEF + (6.0 * COEF * CUBIC) * q))
        a = a.astype(BF16)
        act[j, rows, :] = a
        slp[j, rows, :] = slope.astype(BF16)
        return a

    def store_own(t):
        return pltpu.make_async_copy(
            pbuf.at[0, pl.ds(t * TILE, TILE)], out.at[0, pl.ds(mine + t * TILE, TILE)], s_out.at[t]
        )

    def send_prediction(t):
        return remote(
            pbuf.at[1, pl.ds(t * TILE, TILE)],
            out.at[0, pl.ds(mine + t * TILE, TILE)],
            s_prd.at[t],
            r_prd.at[t],
            pair,
        )

    def own_hidden(t, carry):
        for j in range(4):
            hidden(j, 0, t)
        return carry

    def partner_hidden(t, carry):
        for j in range(4):
            hidden(j, 1, t)
        return carry

    def own_out(t, carry):
        x = lat[0, tile_of(0, t), :].astype(F32)
        for j in range(4):
            x = x + dot(act[j, tile_of(0, t), :], w_out_rows(j))
        pbuf[0, tile_of(0, t), :] = x.astype(BF16)
        store_own(t).start()
        return carry

    lax.fori_loop(0, 2, own_hidden, 0)
    for s in range(2, 4):
        gather_forward(s, 1)
    normalise(1, 2, other_gain, other_shift)
    lax.fori_loop(2, TILES, own_hidden, 0)
    normalise(1, 3, other_gain, other_shift)
    lax.fori_loop(0, 1, partner_hidden, 0)
    for s in range(2, 4):
        gather_end(s, 1)
        share(s, c).start()
    lax.fori_loop(1, TILES, partner_hidden, 0)
    for s in range(2, 4):
        share(s, 1 - c).wait_recv()
    lax.fori_loop(0, TILES, own_out, 0)

    load_target.wait()
    cr[0] = jnp.zeros((8, 128), F32)
    scale = float((2 * NODES) ** -0.5)

    def out_tile(t):
        x = lat[1, tile_of(0, t), :].astype(F32)
        for j in range(4):
            x = x + dot(act[j, tile_of(1, t), :], w_out_rows(j))
        pbuf[1, tile_of(0, t), :] = x.astype(BF16)
        send_prediction(t).start()

    def loss_part(t, k):
        rows = pl.ds(t * TILE + 128 * k, 128)
        p0 = pbuf[0, rows, :].astype(F32)
        p1 = pbuf[1, rows, :].astype(F32)
        goal = tgt[rows, :].astype(F32)
        near0, near1, apart = p0 - goal, p1 - goal, p0 - p1
        q0, q1, qa = near0 * near0 + 0.0625, near1 * near1 + 0.0625, apart * apart + 0.0625
        i0, i1, ia = lax.rsqrt(q0), lax.rsqrt(q1), lax.rsqrt(qa)
        crps = q0 * i0 + q1 * i1 - qa * ia
        summed = jnp.sum(crps.reshape(16, 8, D), axis=0)
        cr[0] += sum(summed[:, n * 128 : (n + 1) * 128] for n in range(4))
        pull = (0.5 * scale) * (apart * ia)
        grads = ((0.5 * scale) * (near0 * i0) - pull, (0.5 * scale) * (near1 * i1) + pull)
        for slot in range(2):
            at = slot * TILE + 128 * k
            (dp0, dp1)[t % 2][at : at + 128, :] = grads[slot].astype(BF16)
            dt[:, pl.ds(slot * HALF + t * TILE + 128 * k, 128)] = grads[slot].T.astype(BF16)

    def back(t, j):
        dact = dot_t((dp0, dp1)[t % 2][...], w_out_rows(j))
        for slot in range(2):
            at = tile_of(slot, t)
            part = dact[slot * TILE : slot * TILE + TILE]
            slp[j, at, :] = (part * slp[j, at, :].astype(F32)).astype(BF16)

    for t in range(TILES + 1):
        if t < TILES:
            out_tile(t)
        for j in range(4):
            if t > 0:
                back(t - 1, j)
            if t < TILES and j < 2:
                loss_part(t, j)

    mates = [
        sib,
        near,
        pair,
        {Y: y + 1 - 2 * lax.rem(y, 2)},
        {Y: 3 - y},
        {Z: z + 1 - 2 * lax.rem(z, 2)},
        {Z: 3 - z},
    ]

    def loss_copy(n):
        return remote(cr.at[n], crr.at[n], s_cr.at[n], r_cr.at[n], mates[n])

    def loss_next(n):
        loss_copy(n).wait()
        cr[n + 1] = cr[n] + crr[n]
        if n + 1 < len(mates):
            loss_copy(n + 1).start()

    blocks = [lax.rem(z + 2, 4), lax.rem(z + 1, 4), lax.rem(z + 3, 4), z]

    def core_copy(n, s, half):
        j, k = blocks[s], 2 * s + half
        if n == 0:
            at = 2 * j + half
            return remote(si.at[1 - c, at], ri.at[at], s_core.at[0, k], r_core.at[0, k], sib)
        ys = pl.ds(2 * half, 2)
        return remote(so.at[1 - c, j, ys], ro.at[j, ys], s_core.at[1, k], r_core.at[1, k], sib)

    def i_block(s):
        j = blocks[s]
        gi = dot(nt[...], slp[j]).reshape(32, 2, 8, 512)
        for half in range(2):
            for core in range(2):
                part = gi[:, core, :, 256 * half : 256 * half + 256]
                si[core, 2 * j + half] = part.reshape(4, 4, 16, 256).astype(BF16)
        for half in range(2):
            core_copy(0, s, half).start()

    def o_block(s):
        j = blocks[s]
        go = dot(dt[...], act[j]).T.reshape(4, 2, 2, 32, 512)
        for core in range(2):
            so[core, j] = go[:, :, core].reshape(4, 64, 512).astype(BF16)
        for half in range(2):
            core_copy(1, s, half).start()

    def i_add(s):
        for half in range(2):
            core_copy(0, s, half).wait_recv()
            k = 2 * blocks[s] + half
            si[c, k] = (si[c, k].astype(F32) + ri[k].astype(F32)).astype(BF16)

    def o_add(s):
        j = blocks[s]
        for half in range(2):
            core_copy(1, s, half).wait_recv()
            ys = pl.ds(2 * half, 2)
            so[c, j, ys] = (so[c, j, ys].astype(F32) + ro[j, ys].astype(F32)).astype(BF16)

    class Ring:
        def __init__(self, n, axis, view, hr, hq, fr, fq):
            p = place[axis]
            q, r, o = lax.rem(p + 1, 4), lax.rem(p + 3, 4), lax.rem(p + 2, 4)
            self.n, self.axis, self.view, self.p, self.q, self.r = n, axis, view, p, q, r
            self.hr, self.hq, self.fr, self.fq = hr, hq, fr, fq
            self.moves = [
                (view(o, 0), hr, up),
                (view(o, 1), hq, down),
                (view(q, 1), fr.at[1], up),
                (view(r, 0), fq.at[0], down),
                (view(q, 0), fr.at[0], up),
                (view(r, 1), fq.at[1], down),
            ]

        def move(self, k):
            src, dst, who = self.moves[k]
            return remote(src, dst, s_rs.at[self.n, k], r_rs.at[self.n, k], who[self.axis])

        def start(self, *ks):
            for k in ks:
                self.move(k).start()

        def relay(self, k):
            i, part, got = [(self.q, 0, self.hr), (self.r, 1, self.hq)][k]
            self.move(k).wait_recv()
            block = self.view(i, part)
            block[...] = (block[...].astype(F32) + got[...].astype(F32)).astype(BF16)
            self.move(4 + k).start()

        def begin(self):
            self.start(0, 1, 2, 3)

        def middle(self):
            self.relay(0)
            self.relay(1)

        def end(self):
            for k in (2, 3, 4, 5):
                self.move(k).wait_recv()
            return [
                self.view(self.p, part)[...].astype(F32)
                + (self.fr[part].astype(F32) + self.fq[part].astype(F32))
                for part in range(2)
            ]

        def drain(self):
            for k in range(6):
                self.move(k).wait_send()

    def i_ring(s):
        return Ring(
            s, Y, lambda i, part: si.at[c, 2 * blocks[s] + part, :, i],
            ihr.at[s], ihq.at[s], ifr.at[s], ifq.at[s],
        )

    i1 = [i_ring(s) for s in range(4)]
    i2 = Ring(4, Z, lambda i, part: ic.at[pl.ds(4 * part, 4), i], jhr, jhq, jfr, jfq)
    o1 = Ring(5, Z, lambda i, part: so.at[c, i, :, pl.ds(32 * part, 32)], ohr, ohq, ofr, ofq)
    o2 = Ring(6, Y, lambda i, part: oc.at[i, pl.ds(32 * part, 32)], phr, phq, pfr, pfq)

    def i_end(s):
        for part, v in enumerate(i1[s].end()):
            ic[2 * blocks[s] + part] = v.astype(BF16)

    far = {X: 1 - h}

    def x_copies(n, send, got):
        ends = [(near, 1 - h), (far, 1 - h), (pair, h)]
        return [
            remote(send.at[part], got.at[k], s_x.at[n, k], r_x.at[n, k], who)
            for k, (who, part) in enumerate(ends)
        ]

    x_i, x_o = x_copies(0, xi, xir), x_copies(1, xo, xor)

    def x_sum(copies, send, got):
        for copy in copies:
            copy.wait_recv()
        own, beside, across, mate = [v.astype(F32) for v in (send[h], got[0], got[1], got[2])]
        return (own + beside) + (mate + across)

    loss_copy(0).start()
    o_block(0)
    i_block(0)
    o_add(0)
    o1.start(0, 1)
    i_block(1)
    i_add(0)
    i1[0].begin()
    i_block(2)
    i_add(1)
    i1[1].begin()
    loss_next(0)
    i_block(3)
    i_add(2)
    i1[2].begin()
    o_block(1)
    i_add(3)
    i1[3].begin()
    loss_next(1)
    o_block(2)
    i1[0].middle()
    o_add(1)
    o1.start(2)
    o1.relay(0)
    o_block(3)
    i1[1].middle()
    o_add(2)
    o1.start(3)
    o1.relay(1)
    loss_next(2)
    i1[2].middle()
    o_add(3)
    i_end(0)
    i1[3].middle()
    i_end(1)
    loss_next(3)
    i_end(2)
    i_end(3)
    i2.begin()
    for part, v in enumerate(o1.end()):
        oc[:, 32 * part : 32 * part + 32] = v.astype(BF16)
    o2.begin()
    loss_next(4)
    i2.middle()
    o2.middle()
    loss_next(5)
    sums = i2.end()
    for half in range(2):
        for part in range(2):
            xi[half, 4 * part : 4 * part + 4] = sums[part][:, 8 * half : 8 * half + 8].astype(BF16)
    for copy in x_i:
        copy.start()
    for part, v in enumerate(o2.end()):
        xo[part] = v.astype(BF16)
    for copy in x_o:
        copy.start()
    loss_next(6)
    loss[0, 0] = jnp.sum(cr[7]) * (0.5 / float(2 * NODES * D))
    total = x_sum(x_i, xi, xir)
    for k in range(8):
        g_in[:, 256 * k : 256 * k + 256] = total[k]
    g_out[...] = x_sum(x_o, xo, xor)

    for copy in first_sends + x_i + x_o:
        copy.wait_send()
    for s in range(4):
        gather_drain(s, 0)
        gather_drain(s, 1)
        share(s, c).wait_send()
        for n in range(2):
            for half in range(2):
                core_copy(n, s, half).wait_send()
    for ring in i1 + [i2, o1, o2]:
        ring.drain()
    for t in range(TILES):
        store_own(t).wait()
        send_latents(t).wait_send()
        send_prediction(t).wait_send()
        remote(
            pbuf.at[1, pl.ds(t * TILE, TILE)],
            out.at[0, pl.ds(theirs + t * TILE, TILE)],
            s_prd.at[t],
            r_prd.at[t],
            pair,
        ).wait_recv()


def finish(p_in, gi_in, go_in, p_out, gi_out, go_out, held, gi, go, s_in, s_out):
    routes = [(gi_in, gi, gi_out), (go_in, go, go_out)]
    for k in range(8):
        part = pl.ds(256 * k, 256)
        routes.append((p_in.at[0, part], held.at[part], p_out.at[0, part]))
    loads = [pltpu.make_async_copy(a, b, s_in.at[k]) for k, (a, b, _) in enumerate(routes)]
    stores = [pltpu.make_async_copy(b, d, s_out.at[k]) for k, (_, b, d) in enumerate(routes)]
    for load in loads:
        load.start()
    for load, store in zip(loads, stores):
        load.wait()
        store.start()
    for store in stores:
        store.wait()


def vm(*shape, dtype=BF16):
    return pltpu.VMEM(shape, dtype)


def dma(*shape):
    return pltpu.SemaphoreType.DMA(shape)


SCRATCH = [
    vm(4, 4, 4, 32, 512), vm(4, 4, 4, 128, 128), vm(2, HALF, D), vm(HALF, D), vm(2, HALF, D),
    vm(2, HALF, D), vm(D, ROWS), vm(2 * TILE, D), vm(2 * TILE, D), vm(D, ROWS), vm(4, ROWS, 512), vm(4, ROWS, 512), vm(1, 32, dtype=F32),
    vm(2, 8, 4, 4, 16, 256), vm(2, 4, 4, 64, 512), vm(8, 4, 4, 16, 256), vm(4, 4, 64, 512),
    vm(4, 4, 16, 256), vm(4, 4, 16, 256), vm(4, 2, 4, 16, 256), vm(4, 2, 4, 16, 256),
    vm(4, 32, 512), vm(4, 32, 512), vm(2, 4, 32, 512), vm(2, 4, 32, 512),
    vm(8, 4, 16, 256), vm(4, 64, 512),
    vm(4, 16, 256), vm(4, 16, 256), vm(2, 4, 16, 256), vm(2, 4, 16, 256),
    vm(32, 512), vm(32, 512), vm(2, 32, 512), vm(2, 32, 512),
    vm(2, 8, 8, 256), vm(3, 8, 8, 256), vm(2, 32, 512), vm(3, 32, 512),
    vm(8, 8, 128, dtype=F32), vm(7, 8, 128, dtype=F32),
    dma(TILES + 1), dma(TILES), dma(TILES), dma(TILES), dma(TILES), dma(TILES),
    pltpu.SemaphoreType.DMA, pltpu.SemaphoreType.DMA,
    dma(3, 4), dma(3, 4), dma(4), dma(4, 2, 4), dma(4, 2, 4), dma(4), dma(4), dma(2, 8), dma(2, 8),
    dma(7, 6), dma(7, 6), dma(2, 3), dma(2, 3), dma(7), dma(7),
]


def on_device(latents, noise, cond_gain, cond_shift, w_in, b_in, w_out, target):
    inside = pl.BlockSpec(memory_space=pltpu.VMEM)
    anywhere = pl.BlockSpec(memory_space=pl.ANY)
    prediction, grad_in, grad_out, loss = pl.pallas_call(
        kernel,
        out_shape=(
            jax.ShapeDtypeStruct((1, ROWS, D), BF16),
            jax.ShapeDtypeStruct((8, H), F32),
            jax.ShapeDtypeStruct((32, D), F32),
            jax.ShapeDtypeStruct((1, 1), F32),
        ),
        in_specs=[anywhere] + [inside] * 6 + [anywhere],
        out_specs=(anywhere, inside, inside, pl.BlockSpec(memory_space=pltpu.SMEM)),
        scratch_shapes=SCRATCH,
        compiler_params=pltpu.CompilerParams(
            collective_id=0, has_side_effects=True, vmem_limit_bytes=63 * 1024 * 1024
        ),
    )(latents, noise, cond_gain, cond_shift, w_in, b_in.reshape(1, H), w_out, target)
    prediction, grad_in, grad_out = pl.pallas_call(
        finish,
        out_shape=(
            jax.ShapeDtypeStruct((1, ROWS, D), BF16),
            jax.ShapeDtypeStruct((8, H), F32),
            jax.ShapeDtypeStruct((32, D), F32),
        ),
        in_specs=[anywhere] * 3,
        out_specs=(anywhere,) * 3,
        scratch_shapes=[vm(ROWS, D), vm(8, H, dtype=F32), vm(32, D, dtype=F32), dma(10), dma(10)],
    )(prediction, grad_in, grad_out)
    return prediction, grad_in, grad_out, loss.reshape(())


def solution(mesh):
    torus = Mesh(mesh.devices.reshape(2, 4, 4, 2, 2), AXES)
    in_specs = (
        P(M, FSDP, None),
        P(M, None),
        P(),
        P(),
        P(FSDP, None),
        P(),
        P(FSDP, None),
        P(FSDP, None),
    )
    out_specs = (P(M, FSDP, None), P(FSDP, None), P(FSDP, None), P())
    return jax.shard_map(on_device, mesh=torus, in_specs=in_specs, out_specs=out_specs, check_vma=False)
```

```python
import jax
import jax.numpy as jnp
from jax import lax
from jax.experimental import pallas as pl
from jax.experimental.pallas import tpu as pltpu
from jax.sharding import Mesh
from jax.sharding import PartitionSpec as P

M, Z, Y, X, C = AXES = ("member", "fsdp_0", "fsdp_1", "fsdp_2", "fsdp_3")
FSDP = (Z, Y, X, C)
MESH = pl.DeviceIdType.MESH
F32 = jnp.float32
BF16 = jnp.bfloat16

COEF = 0.7978845608
CUBIC = 0.044715

D = 512
H = 2048
ROWS = 2048
HALF = 1024
NODES = 131072
TILE = 256
TILES = HALF // TILE


def remote(src, dst, send, recv, device):
    return pltpu.make_async_remote_copy(
        src_ref=src, dst_ref=dst, send_sem=send, recv_sem=recv, device_id=device, device_id_type=MESH
    )


def dot(a, b):
    return jnp.dot(a, b, preferred_element_type=F32)


def dot_t(a, b):
    return lax.dot_general(a, b, (((1,), (1,)), ((), ())), preferred_element_type=F32)


def gain_of(noise, cond):
    n = noise.shape[1]
    square = (n, n)
    same = lax.broadcasted_iota(jnp.int32, square, 0) == lax.broadcasted_iota(jnp.int32, square, 1)
    column = jnp.sum(jnp.where(same, jnp.broadcast_to(noise, square), 0.0), axis=1, keepdims=True)
    return jnp.sum(column * cond, axis=0, keepdims=True)


def kernel(
    latents, noise, cond_gain, cond_shift, w_in, b_in, w_out, target,
    out, g_in, g_out, loss,
    wi, wo, lat, tgt, pbuf, nrm, nt, dp0, dp1, dt, act, slp, nz,
    si, so, ri, ro, ihr, ihq, ifr, ifq, ohr, ohq, ofr, ofq,
    ic, oc, jhr, jhq, jfr, jfq, phr, phq, pfr, pfq,
    xi, xir, xo, xor, cr, crr,
    s_ld, s_out, s_lat, r_lat, s_prd, r_prd, s_nz, r_nz,
    s_w0, r_w0, l_w0, s_ag, r_ag, s_sib, r_sib, s_core, r_core, s_rs, r_rs, s_x, r_x, s_cr, r_cr,
):
    m, z, y, h, c = [lax.axis_index(a) for a in AXES]
    up = {Y: {Y: lax.rem(y + 1, 4)}, Z: {Z: lax.rem(z + 1, 4)}}
    down = {Y: {Y: lax.rem(y + 3, 4)}, Z: {Z: lax.rem(z + 3, 4)}}
    away = {Y: {Y: lax.rem(y + 2, 4)}, Z: {Z: lax.rem(z + 2, 4)}}
    place = {Y: y, Z: z}
    sib = {C: 1 - c}
    pair = {M: 1 - m}
    near = {X: 1 - h, M: 1 - m}
    cross = {X: 1 - h, M: 1 - m, C: 1 - c}

    mine, theirs = m * HALF, (1 - m) * HALF

    def load_own(t):
        return pltpu.make_async_copy(
            latents.at[0, pl.ds(mine + t * TILE, TILE)], lat.at[0, pl.ds(t * TILE, TILE)], s_ld.at[t]
        )

    load_target = pltpu.make_async_copy(target.at[pl.ds(mine, HALF)], tgt, s_ld.at[TILES])
    for t in range(TILES):
        load_own(t).start()
    load_target.start()

    barrier = pltpu.get_barrier_semaphore()
    greeted = [sib, pair, near, cross, {X: 1 - h}, away[Y], away[Z], up[Y], down[Y], up[Z], down[Z]]
    for other in greeted:
        pl.semaphore_signal(barrier, inc=1, device_id=other, device_id_type=MESH)
    pl.semaphore_wait(barrier, len(greeted))

    def shard_parts(h_from, c_from, c_to):
        row = 2 * h_from + c_from
        parts = []
        for k in range(2):
            col = pl.ds(pl.multiple_of(c_to * 1024 + k * 512, 512), 512)
            parts.append((w_in.at[:, col], wi.at[2 * c_to + k, z, y, pl.ds(8 * row, 8)]))
        for k in range(2):
            col = pl.ds(pl.multiple_of(c_to * 256 + k * 128, 128), 128)
            parts.append((w_out.at[:, col], wo.at[2 * c_to + k, z, y, pl.ds(32 * row, 32)]))
        return parts

    partners = [(near, 1 - h, c), (cross, 1 - h, 1 - c), (sib, h, 1 - c)]
    first_sends = []
    for n, (src, dst) in enumerate(shard_parts(h, c, c)):
        pltpu.make_async_copy(src, dst, l_w0.at[n]).start()
    for n in range(4):
        for r, (who, _, c_to) in enumerate(partners):
            src, dst = shard_parts(h, c, c_to)[n]
            copy = remote(src, dst, s_w0.at[r, n], r_w0.at[r, n], who)
            copy.start()
            first_sends.append(copy)

    noise_copy = remote(noise, nz, s_nz, r_nz, pair)
    noise_copy.start()

    def send_latents(t):
        return remote(
            latents.at[0, pl.ds(theirs + t * TILE, TILE)],
            lat.at[1, pl.ds(t * TILE, TILE)],
            s_lat.at[t],
            r_lat.at[t],
            pair,
        )

    for t in range(TILES):
        send_latents(t).start()

    def tile_of(slot, t):
        return pl.ds(pl.multiple_of(slot * HALF + t * TILE, TILE), TILE)

    def normalise(slot, t, gain, shift):
        if slot == 0:
            load_own(t).wait()
        else:
            send_latents(t).wait_recv()
        x = lat[slot, tile_of(0, t), :].astype(F32)
        centred = x - jnp.mean(x, axis=1, keepdims=True)
        spread = jnp.mean(centred * centred, axis=1, keepdims=True)
        normed = centred * lax.rsqrt(spread + 0.25) * gain + shift
        nt[:, tile_of(slot, t)] = normed.T.astype(BF16)
        nrm[slot, tile_of(0, t), :] = normed.astype(BF16)

    gain, shift = 1.0 + gain_of(noise[...], cond_gain[...]), gain_of(noise[...], cond_shift[...])
    for t in range(2):
        normalise(0, t, gain, shift)
    streams = [(wi, 0, Y), (wi, 1, Z), (wo, 0, Y), (wo, 1, Z)]

    def other_axis(a):
        return Z if a == Y else Y

    def gather_view(s, phase, i, part):
        ref, k, first = streams[s]
        size = ref.shape[3]
        rows = pl.ds(0, size) if part is None else pl.ds(part * size // 2, size // 2)
        block = 2 * c + k
        if phase == 0:
            return ref.at[block, z, i, rows] if first == Y else ref.at[block, i, y, rows]
        return ref.at[block, i, :, rows] if first == Y else ref.at[block, :, i, rows]

    def gather_copy(s, phase, n):
        axis = streams[s][2] if phase == 0 else other_axis(streams[s][2])
        p = place[axis]
        if phase == 0:
            i, part, who = p, None, [up, down, away][n][axis]
        else:
            i = [p, p, lax.rem(p + 3, 4), lax.rem(p + 1, 4)][n]
            part, who = [None, None, 0, 1][n], [up, down, up, down][n][axis]
        view = gather_view(s, phase, i, part)
        return remote(view, view, s_ag.at[s, phase, n], r_ag.at[s, phase, n], who)

    def gather_landed(s, phase, n):
        axis = streams[s][2] if phase == 0 else other_axis(streams[s][2])
        p = place[axis]
        i = lax.rem(p + [3, 1, 2, 2][n], 4)
        view = gather_view(s, phase, i, None if phase == 0 else [None, None, 0, 1][n])
        remote(view, view, s_ag.at[s, phase, n], r_ag.at[s, phase, n], up[axis]).wait_recv()

    def gather_start(s, phase):
        for n in range(3 if phase == 0 else 2):
            gather_copy(s, phase, n).start()

    def gather_forward(s, phase):
        if phase == 0:
            return
        gather_landed(s, phase, 0)
        gather_copy(s, phase, 2).start()
        gather_landed(s, phase, 1)
        gather_copy(s, phase, 3).start()

    def gather_end(s, phase):
        for n in range(3) if phase == 0 else (2, 3):
            gather_landed(s, phase, n)

    def gather_drain(s, phase):
        for n in range(3 if phase == 0 else 4):
            gather_copy(s, phase, n).wait_send()

    def share(s, block_of):
        ref, k, _ = streams[s]
        view = ref.at[2 * block_of + k]
        return remote(view, view, s_sib.at[s], r_sib.at[s], sib)

    for n in range(4):
        src, dst = shard_parts(h, c, c)[n]
        pltpu.make_async_copy(src, dst, l_w0.at[n]).wait()
        for r, (who, h_from, c_from) in enumerate(partners):
            src, dst = shard_parts(h_from, c_from, c)[n]
            remote(src, dst, s_w0.at[r, n], r_w0.at[r, n], who).wait_recv()
        gather_start(n, 0)
    normalise(0, 2, gain, shift)
    for s in range(4):
        gather_forward(s, 0)
    normalise(0, 3, gain, shift)
    for s in range(2):
        gather_end(s, 0)
        gather_start(s, 1)
    noise_copy.wait()
    other_gain, other_shift = 1.0 + gain_of(nz[...], cond_gain[...]), gain_of(nz[...], cond_shift[...])
    normalise(1, 0, other_gain, other_shift)
    for s in range(2):
        gather_forward(s, 1)
    for s in range(2, 4):
        gather_end(s, 0)
        gather_start(s, 1)
    normalise(1, 1, other_gain, other_shift)
    for s in range(2):
        gather_end(s, 1)
        share(s, c).start()
    for s in range(2):
        share(s, 1 - c).wait_recv()

    def w_out_rows(j):
        return jnp.concatenate([wo[b, j].reshape(512, 128) for b in range(4)], axis=1)

    def hidden(j, slot, t):
        rows = tile_of(slot, t)
        v = dot(nrm[slot, tile_of(0, t), :], wi[j].reshape(512, 512)) + b_in[:, 512 * j : 512 * j + 512]
        q = v * v
        u = jnp.tanh(v * (COEF + (COEF * CUBIC) * q))
        half = 0.5 + 0.5 * u
        a = v * half
        slope = half + a * ((1.0 - half) * (2.0 * COEF + (6.0 * COEF * CUBIC) * q))
        a = a.astype(BF16)
        act[j, rows, :] = a
        slp[j, rows, :] = slope.astype(BF16)
        return a

    def store_own(t):
        return pltpu.make_async_copy(
            pbuf.at[0, pl.ds(t * TILE, TILE)], out.at[0, pl.ds(mine + t * TILE, TILE)], s_out.at[t]
        )

    def send_prediction(t):
        return remote(
            pbuf.at[1, pl.ds(t * TILE, TILE)],
            out.at[0, pl.ds(mine + t * TILE, TILE)],
            s_prd.at[t],
            r_prd.at[t],
            pair,
        )

    def own_hidden(t, carry):
        for j in range(4):
            hidden(j, 0, t)
        return carry

    def partner_hidden(t, carry):
        for j in range(4):
            hidden(j, 1, t)
        return carry

    def own_out(t, beside):
        x = lat[0, tile_of(0, t), :].astype(F32)
        for j in range(4):
            x = x + dot(act[j, tile_of(0, t), :], w_out_rows(j))
            if beside is not None:
                hidden(j, 1, beside)
        pbuf[0, tile_of(0, t), :] = x.astype(BF16)
        store_own(t).start()

    lax.fori_loop(0, 1, own_hidden, 0)
    for s in range(2, 4):
        gather_forward(s, 1)
    lax.fori_loop(1, TILES, own_hidden, 0)
    for t in range(2, TILES):
        normalise(1, t, other_gain, other_shift)
    for s in range(2, 4):
        gather_end(s, 1)
        share(s, c).start()
    lax.fori_loop(0, 2, partner_hidden, 0)
    for s in range(2, 4):
        share(s, 1 - c).wait_recv()
    for t in range(TILES):
        own_out(t, t + 2 if t + 2 < TILES else None)

    load_target.wait()
    cr[0] = jnp.zeros((8, 128), F32)
    scale = float((2 * NODES) ** -0.5)

    def out_tile(t):
        x = lat[1, tile_of(0, t), :].astype(F32)
        for j in range(4):
            x = x + dot(act[j, tile_of(1, t), :], w_out_rows(j))
        pbuf[1, tile_of(0, t), :] = x.astype(BF16)
        send_prediction(t).start()

    def loss_part(t, k):
        rows = pl.ds(t * TILE + 128 * k, 128)
        p0 = pbuf[0, rows, :].astype(F32)
        p1 = pbuf[1, rows, :].astype(F32)
        goal = tgt[rows, :].astype(F32)
        near0, near1, apart = p0 - goal, p1 - goal, p0 - p1
        q0, q1, qa = near0 * near0 + 0.0625, near1 * near1 + 0.0625, apart * apart + 0.0625
        i0, i1, ia = lax.rsqrt(q0), lax.rsqrt(q1), lax.rsqrt(qa)
        crps = q0 * i0 + q1 * i1 - qa * ia
        summed = jnp.sum(crps.reshape(16, 8, D), axis=0)
        cr[0] += sum(summed[:, n * 128 : (n + 1) * 128] for n in range(4))
        pull = (0.5 * scale) * (apart * ia)
        grads = ((0.5 * scale) * (near0 * i0) - pull, (0.5 * scale) * (near1 * i1) + pull)
        for slot in range(2):
            at = slot * TILE + 128 * k
            (dp0, dp1)[t % 2][at : at + 128, :] = grads[slot].astype(BF16)
            dt[:, pl.ds(slot * HALF + t * TILE + 128 * k, 128)] = grads[slot].T.astype(BF16)

    def back(t, j):
        dact = dot_t((dp0, dp1)[t % 2][...], w_out_rows(j))
        for slot in range(2):
            at = tile_of(slot, t)
            part = dact[slot * TILE : slot * TILE + TILE]
            slp[j, at, :] = (part * slp[j, at, :].astype(F32)).astype(BF16)

    for t in range(TILES + 1):
        if t < TILES:
            out_tile(t)
        for j in range(4):
            if t > 0:
                back(t - 1, j)
            if t < TILES and j < 2:
                loss_part(t, j)

    mates = [
        sib,
        near,
        pair,
        {Y: y + 1 - 2 * lax.rem(y, 2)},
        {Y: 3 - y},
        {Z: z + 1 - 2 * lax.rem(z, 2)},
        {Z: 3 - z},
    ]

    def loss_copy(n):
        return remote(cr.at[n], crr.at[n], s_cr.at[n], r_cr.at[n], mates[n])

    def loss_next(n):
        loss_copy(n).wait()
        cr[n + 1] = cr[n] + crr[n]
        if n + 1 < len(mates):
            loss_copy(n + 1).start()

    blocks = [lax.rem(z + 2, 4), lax.rem(z + 1, 4), lax.rem(z + 3, 4), z]

    def core_copy(n, s, half):
        j, k = blocks[s], 2 * s + half
        if n == 0:
            at = 2 * j + half
            return remote(si.at[1 - c, at], ri.at[at], s_core.at[0, k], r_core.at[0, k], sib)
        ys = pl.ds(2 * half, 2)
        return remote(so.at[1 - c, j, ys], ro.at[j, ys], s_core.at[1, k], r_core.at[1, k], sib)

    def i_block(s):
        j = blocks[s]
        gi = dot(nt[...], slp[j]).reshape(32, 2, 8, 512)
        for half in range(2):
            for core in range(2):
                part = gi[:, core, :, 256 * half : 256 * half + 256]
                si[core, 2 * j + half] = part.reshape(4, 4, 16, 256).astype(BF16)
        for half in range(2):
            core_copy(0, s, half).start()

    def o_block(s):
        j = blocks[s]
        go = dot(dt[...], act[j]).T.reshape(4, 2, 2, 32, 512)
        for core in range(2):
            so[core, j] = go[:, :, core].reshape(4, 64, 512).astype(BF16)
        for half in range(2):
            core_copy(1, s, half).start()

    def i_add(s):
        for half in range(2):
            core_copy(0, s, half).wait_recv()
            k = 2 * blocks[s] + half
            si[c, k] = (si[c, k].astype(F32) + ri[k].astype(F32)).astype(BF16)

    def o_add(s):
        j = blocks[s]
        for half in range(2):
            core_copy(1, s, half).wait_recv()
            ys = pl.ds(2 * half, 2)
            so[c, j, ys] = (so[c, j, ys].astype(F32) + ro[j, ys].astype(F32)).astype(BF16)

    class Ring:
        def __init__(self, n, axis, view, hr, hq, fr, fq):
            p = place[axis]
            q, r, o = lax.rem(p + 1, 4), lax.rem(p + 3, 4), lax.rem(p + 2, 4)
            self.n, self.axis, self.view, self.p, self.q, self.r = n, axis, view, p, q, r
            self.hr, self.hq, self.fr, self.fq = hr, hq, fr, fq
            self.moves = [
                (view(o, 0), hr, up),
                (view(o, 1), hq, down),
                (view(q, 1), fr.at[1], up),
                (view(r, 0), fq.at[0], down),
                (view(q, 0), fr.at[0], up),
                (view(r, 1), fq.at[1], down),
            ]

        def move(self, k):
            src, dst, who = self.moves[k]
            return remote(src, dst, s_rs.at[self.n, k], r_rs.at[self.n, k], who[self.axis])

        def start(self, *ks):
            for k in ks:
                self.move(k).start()

        def relay(self, k):
            i, part, got = [(self.q, 0, self.hr), (self.r, 1, self.hq)][k]
            self.move(k).wait_recv()
            block = self.view(i, part)
            block[...] = (block[...].astype(F32) + got[...].astype(F32)).astype(BF16)
            self.move(4 + k).start()

        def begin(self):
            self.start(0, 1, 2, 3)

        def middle(self):
            self.relay(0)
            self.relay(1)

        def end(self):
            for k in (2, 3, 4, 5):
                self.move(k).wait_recv()
            return [
                self.view(self.p, part)[...].astype(F32)
                + (self.fr[part].astype(F32) + self.fq[part].astype(F32))
                for part in range(2)
            ]

        def drain(self):
            for k in range(6):
                self.move(k).wait_send()

    def i_ring(s):
        return Ring(
            s, Y, lambda i, part: si.at[c, 2 * blocks[s] + part, :, i],
            ihr.at[s], ihq.at[s], ifr.at[s], ifq.at[s],
        )

    i1 = [i_ring(s) for s in range(4)]
    i2 = Ring(4, Z, lambda i, part: ic.at[pl.ds(4 * part, 4), i], jhr, jhq, jfr, jfq)
    o1 = Ring(5, Z, lambda i, part: so.at[c, i, :, pl.ds(32 * part, 32)], ohr, ohq, ofr, ofq)
    o2 = Ring(6, Y, lambda i, part: oc.at[i, pl.ds(32 * part, 32)], phr, phq, pfr, pfq)

    def i_end(s):
        for part, v in enumerate(i1[s].end()):
            ic[2 * blocks[s] + part] = v.astype(BF16)

    far = {X: 1 - h}

    def x_copies(n, send, got):
        ends = [(near, 1 - h), (far, 1 - h), (pair, h)]
        return [
            remote(send.at[part], got.at[k], s_x.at[n, k], r_x.at[n, k], who)
            for k, (who, part) in enumerate(ends)
        ]

    x_i, x_o = x_copies(0, xi, xir), x_copies(1, xo, xor)

    def x_sum(copies, send, got):
        for copy in copies:
            copy.wait_recv()
        own, beside, across, mate = [v.astype(F32) for v in (send[h], got[0], got[1], got[2])]
        return (own + beside) + (mate + across)

    loss_copy(0).start()
    o_block(0)
    i_block(0)
    o_add(0)
    o1.start(0, 1)
    i_block(1)
    i_add(0)
    i1[0].begin()
    i_block(2)
    i_add(1)
    i1[1].begin()
    i_block(3)
    i_add(2)
    i1[2].begin()
    loss_next(0)
    o_block(1)
    i_add(3)
    i1[3].begin()
    o_block(2)
    o_add(1)
    o1.start(2)
    i1[0].middle()
    o1.relay(0)
    loss_next(1)
    o_block(3)
    o_add(2)
    o1.start(3)
    o1.relay(1)
    i1[1].middle()
    i1[2].middle()
    o_add(3)
    i1[3].middle()
    loss_next(2)
    i_end(0)
    i_end(1)
    i_end(2)
    loss_next(3)
    i_end(3)
    i2.begin()
    for part, v in enumerate(o1.end()):
        oc[:, 32 * part : 32 * part + 32] = v.astype(BF16)
    o2.begin()
    loss_next(4)
    i2.middle()
    o2.middle()
    loss_next(5)
    sums = i2.end()
    for half in range(2):
        for part in range(2):
            xi[half, 4 * part : 4 * part + 4] = sums[part][:, 8 * half : 8 * half + 8].astype(BF16)
    for copy in x_i:
        copy.start()
    for part, v in enumerate(o2.end()):
        xo[part] = v.astype(BF16)
    for copy in x_o:
        copy.start()
    loss_next(6)
    loss[0, 0] = jnp.sum(cr[7]) * (0.5 / float(2 * NODES * D))
    total = x_sum(x_i, xi, xir)
    for k in range(8):
        g_in[:, 256 * k : 256 * k + 256] = total[k]
    g_out[...] = x_sum(x_o, xo, xor)

    for copy in first_sends + x_i + x_o:
        copy.wait_send()
    for s in range(4):
        gather_drain(s, 0)
        gather_drain(s, 1)
        share(s, c).wait_send()
        for n in range(2):
            for half in range(2):
                core_copy(n, s, half).wait_send()
    for ring in i1 + [i2, o1, o2]:
        ring.drain()
    for t in range(TILES):
        store_own(t).wait()
        send_latents(t).wait_send()
        send_prediction(t).wait_send()
        remote(
            pbuf.at[1, pl.ds(t * TILE, TILE)],
            out.at[0, pl.ds(theirs + t * TILE, TILE)],
            s_prd.at[t],
            r_prd.at[t],
            pair,
        ).wait_recv()


def finish(p_in, gi_in, go_in, p_out, gi_out, go_out, held, gi, go, s_in, s_out):
    routes = [(gi_in, gi, gi_out), (go_in, go, go_out)]
    for k in range(8):
        part = pl.ds(256 * k, 256)
        routes.append((p_in.at[0, part], held.at[part], p_out.at[0, part]))
    loads = [pltpu.make_async_copy(a, b, s_in.at[k]) for k, (a, b, _) in enumerate(routes)]
    stores = [pltpu.make_async_copy(b, d, s_out.at[k]) for k, (_, b, d) in enumerate(routes)]
    for load in loads:
        load.start()
    for load, store in zip(loads, stores):
        load.wait()
        store.start()
    for store in stores:
        store.wait()


def vm(*shape, dtype=BF16):
    return pltpu.VMEM(shape, dtype)


def dma(*shape):
    return pltpu.SemaphoreType.DMA(shape)


SCRATCH = [
    vm(4, 4, 4, 32, 512), vm(4, 4, 4, 128, 128), vm(2, HALF, D), vm(HALF, D), vm(2, HALF, D),
    vm(2, HALF, D), vm(D, ROWS), vm(2 * TILE, D), vm(2 * TILE, D), vm(D, ROWS), vm(4, ROWS, 512), vm(4, ROWS, 512), vm(1, 32, dtype=F32),
    vm(2, 8, 4, 4, 16, 256), vm(2, 4, 4, 64, 512), vm(8, 4, 4, 16, 256), vm(4, 4, 64, 512),
    vm(4, 4, 16, 256), vm(4, 4, 16, 256), vm(4, 2, 4, 16, 256), vm(4, 2, 4, 16, 256),
    vm(4, 32, 512), vm(4, 32, 512), vm(2, 4, 32, 512), vm(2, 4, 32, 512),
    vm(8, 4, 16, 256), vm(4, 64, 512),
    vm(4, 16, 256), vm(4, 16, 256), vm(2, 4, 16, 256), vm(2, 4, 16, 256),
    vm(32, 512), vm(32, 512), vm(2, 32, 512), vm(2, 32, 512),
    vm(2, 8, 8, 256), vm(3, 8, 8, 256), vm(2, 32, 512), vm(3, 32, 512),
    vm(8, 8, 128, dtype=F32), vm(7, 8, 128, dtype=F32),
    dma(TILES + 1), dma(TILES), dma(TILES), dma(TILES), dma(TILES), dma(TILES),
    pltpu.SemaphoreType.DMA, pltpu.SemaphoreType.DMA,
    dma(3, 4), dma(3, 4), dma(4), dma(4, 2, 4), dma(4, 2, 4), dma(4), dma(4), dma(2, 8), dma(2, 8),
    dma(7, 6), dma(7, 6), dma(2, 3), dma(2, 3), dma(7), dma(7),
]


def on_device(latents, noise, cond_gain, cond_shift, w_in, b_in, w_out, target):
    inside = pl.BlockSpec(memory_space=pltpu.VMEM)
    anywhere = pl.BlockSpec(memory_space=pl.ANY)
    prediction, grad_in, grad_out, loss = pl.pallas_call(
        kernel,
        out_shape=(
            jax.ShapeDtypeStruct((1, ROWS, D), BF16),
            jax.ShapeDtypeStruct((8, H), F32),
            jax.ShapeDtypeStruct((32, D), F32),
            jax.ShapeDtypeStruct((1, 1), F32),
        ),
        in_specs=[anywhere] + [inside] * 6 + [anywhere],
        out_specs=(anywhere, inside, inside, pl.BlockSpec(memory_space=pltpu.SMEM)),
        scratch_shapes=SCRATCH,
        compiler_params=pltpu.CompilerParams(
            collective_id=0, has_side_effects=True, vmem_limit_bytes=63 * 1024 * 1024
        ),
    )(latents, noise, cond_gain, cond_shift, w_in, b_in.reshape(1, H), w_out, target)
    prediction, grad_in, grad_out = pl.pallas_call(
        finish,
        out_shape=(
            jax.ShapeDtypeStruct((1, ROWS, D), BF16),
            jax.ShapeDtypeStruct((8, H), F32),
            jax.ShapeDtypeStruct((32, D), F32),
        ),
        in_specs=[anywhere] * 3,
        out_specs=(anywhere,) * 3,
        scratch_shapes=[vm(ROWS, D), vm(8, H, dtype=F32), vm(32, D, dtype=F32), dma(10), dma(10)],
    )(prediction, grad_in, grad_out)
    return prediction, grad_in, grad_out, loss.reshape(())


def solution(mesh):
    torus = Mesh(mesh.devices.reshape(2, 4, 4, 2, 2), AXES)
    in_specs = (
        P(M, FSDP, None),
        P(M, None),
        P(),
        P(),
        P(FSDP, None),
        P(),
        P(FSDP, None),
        P(FSDP, None),
    )
    out_specs = (P(M, FSDP, None), P(FSDP, None), P(FSDP, None), P())
    return jax.shard_map(on_device, mesh=torus, in_specs=in_specs, out_specs=out_specs, check_vma=False)
```

```python
import jax
import jax.numpy as jnp
from jax import lax
from jax.experimental import pallas as pl
from jax.experimental.pallas import tpu as pltpu
from jax.sharding import Mesh
from jax.sharding import PartitionSpec as P

M, Z, Y, X, C = AXES = ("member", "fsdp_0", "fsdp_1", "fsdp_2", "fsdp_3")
FSDP = (Z, Y, X, C)
MESH = pl.DeviceIdType.MESH
F32 = jnp.float32
BF16 = jnp.bfloat16

COEF = 0.7978845608
CUBIC = 0.044715

D = 512
H = 2048
ROWS = 2048
HALF = 1024
NODES = 131072
TILE = 256
TILES = HALF // TILE


def remote(src, dst, send, recv, device):
    return pltpu.make_async_remote_copy(
        src_ref=src, dst_ref=dst, send_sem=send, recv_sem=recv, device_id=device, device_id_type=MESH
    )


def dot(a, b):
    return jnp.dot(a, b, preferred_element_type=F32)


def dot_t(a, b):
    return lax.dot_general(a, b, (((1,), (1,)), ((), ())), preferred_element_type=F32)


def gain_of(noise, cond):
    n = noise.shape[1]
    square = (n, n)
    same = lax.broadcasted_iota(jnp.int32, square, 0) == lax.broadcasted_iota(jnp.int32, square, 1)
    column = jnp.sum(jnp.where(same, jnp.broadcast_to(noise, square), 0.0), axis=1, keepdims=True)
    return jnp.sum(column * cond, axis=0, keepdims=True)


def kernel(
    latents, noise, cond_gain, cond_shift, w_in, b_in, w_out, target,
    out, g_in, g_out, loss,
    wi, wo, lat, tgt, pbuf, nrm, nt, dp0, dp1, dt, act, slp, nz,
    si, so, ri, ro, ihr, ihq, ifr, ifq, ohr, ohq, ofr, ofq,
    ic, oc, jgot, pgot,
    xi, xir, xo, xor, cr, crr,
    s_ld, s_out, s_lat, r_lat, s_prd, r_prd, s_nz, r_nz,
    s_w0, r_w0, l_w0, s_ag, r_ag, s_sib, r_sib, s_core, r_core, s_rs, r_rs, s_x, r_x, s_cr, r_cr,
):
    m, z, y, h, c = [lax.axis_index(a) for a in AXES]
    up = {Y: {Y: lax.rem(y + 1, 4)}, Z: {Z: lax.rem(z + 1, 4)}}
    down = {Y: {Y: lax.rem(y + 3, 4)}, Z: {Z: lax.rem(z + 3, 4)}}
    away = {Y: {Y: lax.rem(y + 2, 4)}, Z: {Z: lax.rem(z + 2, 4)}}
    place = {Y: y, Z: z}
    sib = {C: 1 - c}
    pair = {M: 1 - m}
    near = {X: 1 - h, M: 1 - m}
    cross = {X: 1 - h, M: 1 - m, C: 1 - c}

    mine, theirs = m * HALF, (1 - m) * HALF

    def load_own(t):
        return pltpu.make_async_copy(
            latents.at[0, pl.ds(mine + t * TILE, TILE)], lat.at[0, pl.ds(t * TILE, TILE)], s_ld.at[t]
        )

    load_target = pltpu.make_async_copy(target.at[pl.ds(mine, HALF)], tgt, s_ld.at[TILES])
    for t in range(TILES):
        load_own(t).start()
    load_target.start()

    barrier = pltpu.get_barrier_semaphore()
    greeted = [sib, pair, near, cross, {X: 1 - h}, away[Y], away[Z], up[Y], down[Y], up[Z], down[Z]]
    for other in greeted:
        pl.semaphore_signal(barrier, inc=1, device_id=other, device_id_type=MESH)
    pl.semaphore_wait(barrier, len(greeted))

    def shard_parts(h_from, c_from, c_to):
        row = 2 * h_from + c_from
        parts = []
        for k in range(2):
            col = pl.ds(pl.multiple_of(c_to * 1024 + k * 512, 512), 512)
            parts.append((w_in.at[:, col], wi.at[2 * c_to + k, z, y, pl.ds(8 * row, 8)]))
        for k in range(2):
            col = pl.ds(pl.multiple_of(c_to * 256 + k * 128, 128), 128)
            parts.append((w_out.at[:, col], wo.at[2 * c_to + k, z, y, pl.ds(32 * row, 32)]))
        return parts

    partners = [(near, 1 - h, c), (cross, 1 - h, 1 - c), (sib, h, 1 - c)]
    first_sends = []
    for n, (src, dst) in enumerate(shard_parts(h, c, c)):
        pltpu.make_async_copy(src, dst, l_w0.at[n]).start()
    for n in range(4):
        for r, (who, _, c_to) in enumerate(partners):
            src, dst = shard_parts(h, c, c_to)[n]
            copy = remote(src, dst, s_w0.at[r, n], r_w0.at[r, n], who)
            copy.start()
            first_sends.append(copy)

    noise_copy = remote(noise, nz, s_nz, r_nz, pair)
    noise_copy.start()

    def send_latents(t):
        return remote(
            latents.at[0, pl.ds(theirs + t * TILE, TILE)],
            lat.at[1, pl.ds(t * TILE, TILE)],
            s_lat.at[t],
            r_lat.at[t],
            pair,
        )

    for t in range(TILES):
        send_latents(t).start()

    def tile_of(slot, t):
        return pl.ds(pl.multiple_of(slot * HALF + t * TILE, TILE), TILE)

    def normalise(slot, t, gain, shift):
        if slot == 0:
            load_own(t).wait()
        else:
            send_latents(t).wait_recv()
        x = lat[slot, tile_of(0, t), :].astype(F32)
        centred = x - jnp.mean(x, axis=1, keepdims=True)
        spread = jnp.mean(centred * centred, axis=1, keepdims=True)
        normed = centred * lax.rsqrt(spread + 0.25) * gain + shift
        nt[:, tile_of(slot, t)] = normed.T.astype(BF16)
        nrm[slot, tile_of(0, t), :] = normed.astype(BF16)

    gain, shift = 1.0 + gain_of(noise[...], cond_gain[...]), gain_of(noise[...], cond_shift[...])
    for t in range(2):
        normalise(0, t, gain, shift)
    streams = [(wi, 0, Y), (wi, 1, Z), (wo, 0, Y), (wo, 1, Z)]

    def other_axis(a):
        return Z if a == Y else Y

    def gather_view(s, phase, i, part):
        ref, k, first = streams[s]
        size = ref.shape[3]
        rows = pl.ds(0, size) if part is None else pl.ds(part * size // 2, size // 2)
        block = 2 * c + k
        if phase == 0:
            return ref.at[block, z, i, rows] if first == Y else ref.at[block, i, y, rows]
        return ref.at[block, i, :, rows] if first == Y else ref.at[block, :, i, rows]

    def gather_copy(s, phase, n):
        axis = streams[s][2] if phase == 0 else other_axis(streams[s][2])
        p = place[axis]
        if phase == 0:
            i, part, who = p, None, [up, down, away][n][axis]
        else:
            i = [p, p, lax.rem(p + 3, 4), lax.rem(p + 1, 4)][n]
            part, who = [None, None, 0, 1][n], [up, down, up, down][n][axis]
        view = gather_view(s, phase, i, part)
        return remote(view, view, s_ag.at[s, phase, n], r_ag.at[s, phase, n], who)

    def gather_landed(s, phase, n):
        axis = streams[s][2] if phase == 0 else other_axis(streams[s][2])
        p = place[axis]
        i = lax.rem(p + [3, 1, 2, 2][n], 4)
        view = gather_view(s, phase, i, None if phase == 0 else [None, None, 0, 1][n])
        remote(view, view, s_ag.at[s, phase, n], r_ag.at[s, phase, n], up[axis]).wait_recv()

    def gather_start(s, phase):
        for n in range(3 if phase == 0 else 2):
            gather_copy(s, phase, n).start()

    def gather_forward(s, phase):
        if phase == 0:
            return
        gather_landed(s, phase, 0)
        gather_copy(s, phase, 2).start()
        gather_landed(s, phase, 1)
        gather_copy(s, phase, 3).start()

    def gather_end(s, phase):
        for n in range(3) if phase == 0 else (2, 3):
            gather_landed(s, phase, n)

    def gather_drain(s, phase):
        for n in range(3 if phase == 0 else 4):
            gather_copy(s, phase, n).wait_send()

    def share(s, block_of):
        ref, k, _ = streams[s]
        view = ref.at[2 * block_of + k]
        return remote(view, view, s_sib.at[s], r_sib.at[s], sib)

    for n in range(4):
        src, dst = shard_parts(h, c, c)[n]
        pltpu.make_async_copy(src, dst, l_w0.at[n]).wait()
        for r, (who, h_from, c_from) in enumerate(partners):
            src, dst = shard_parts(h_from, c_from, c)[n]
            remote(src, dst, s_w0.at[r, n], r_w0.at[r, n], who).wait_recv()
        gather_start(n, 0)
    normalise(0, 2, gain, shift)
    for s in range(4):
        gather_forward(s, 0)
    normalise(0, 3, gain, shift)
    for s in range(2):
        gather_end(s, 0)
        gather_start(s, 1)
    noise_copy.wait()
    other_gain, other_shift = 1.0 + gain_of(nz[...], cond_gain[...]), gain_of(nz[...], cond_shift[...])
    normalise(1, 0, other_gain, other_shift)
    for s in range(2):
        gather_forward(s, 1)
    for s in range(2, 4):
        gather_end(s, 0)
        gather_start(s, 1)
    normalise(1, 1, other_gain, other_shift)
    for s in range(2):
        gather_end(s, 1)
        share(s, c).start()
    for s in range(2):
        share(s, 1 - c).wait_recv()

    def w_out_rows(j):
        return jnp.concatenate([wo[b, j].reshape(512, 128) for b in range(4)], axis=1)

    def hidden(j, slot, t):
        rows = tile_of(slot, t)
        v = dot(nrm[slot, tile_of(0, t), :], wi[j].reshape(512, 512)) + b_in[:, 512 * j : 512 * j + 512]
        q = v * v
        u = jnp.tanh(v * (COEF + (COEF * CUBIC) * q))
        half = 0.5 + 0.5 * u
        a = v * half
        slope = half + a * ((1.0 - half) * (2.0 * COEF + (6.0 * COEF * CUBIC) * q))
        a = a.astype(BF16)
        act[j, rows, :] = a
        slp[j, rows, :] = slope.astype(BF16)
        return a

    def store_own(t):
        return pltpu.make_async_copy(
            pbuf.at[0, pl.ds(t * TILE, TILE)], out.at[0, pl.ds(mine + t * TILE, TILE)], s_out.at[t]
        )

    def send_prediction(t):
        return remote(
            pbuf.at[1, pl.ds(t * TILE, TILE)],
            out.at[0, pl.ds(mine + t * TILE, TILE)],
            s_prd.at[t],
            r_prd.at[t],
            pair,
        )

    def own_hidden(t, carry):
        for j in range(4):
            hidden(j, 0, t)
        return carry

    def partner_hidden(t, carry):
        for j in range(4):
            hidden(j, 1, t)
        return carry

    def own_out(t, beside):
        x = lat[0, tile_of(0, t), :].astype(F32)
        for j in range(4):
            x = x + dot(act[j, tile_of(0, t), :], w_out_rows(j))
            if beside is not None:
                hidden(j, 1, beside)
        pbuf[0, tile_of(0, t), :] = x.astype(BF16)
        store_own(t).start()

    lax.fori_loop(0, 1, own_hidden, 0)
    for s in range(2, 4):
        gather_forward(s, 1)
    lax.fori_loop(1, TILES, own_hidden, 0)
    for t in range(2, TILES):
        normalise(1, t, other_gain, other_shift)
    for s in range(2, 4):
        gather_end(s, 1)
        share(s, c).start()
    lax.fori_loop(0, 2, partner_hidden, 0)
    for s in range(2, 4):
        share(s, 1 - c).wait_recv()
    for t in range(TILES):
        own_out(t, t + 2 if t + 2 < TILES else None)

    load_target.wait()
    cr[0] = jnp.zeros((8, 128), F32)
    scale = float((2 * NODES) ** -0.5)

    def out_tile(t):
        x = lat[1, tile_of(0, t), :].astype(F32)
        for j in range(4):
            x = x + dot(act[j, tile_of(1, t), :], w_out_rows(j))
        pbuf[1, tile_of(0, t), :] = x.astype(BF16)
        send_prediction(t).start()

    def loss_part(t, k):
        rows = pl.ds(t * TILE + 128 * k, 128)
        p0 = pbuf[0, rows, :].astype(F32)
        p1 = pbuf[1, rows, :].astype(F32)
        goal = tgt[rows, :].astype(F32)
        near0, near1, apart = p0 - goal, p1 - goal, p0 - p1
        q0, q1, qa = near0 * near0 + 0.0625, near1 * near1 + 0.0625, apart * apart + 0.0625
        i0, i1, ia = lax.rsqrt(q0), lax.rsqrt(q1), lax.rsqrt(qa)
        crps = q0 * i0 + q1 * i1 - qa * ia
        summed = jnp.sum(crps.reshape(16, 8, D), axis=0)
        cr[0] += sum(summed[:, n * 128 : (n + 1) * 128] for n in range(4))
        pull = (0.5 * scale) * (apart * ia)
        grads = ((0.5 * scale) * (near0 * i0) - pull, (0.5 * scale) * (near1 * i1) + pull)
        for slot in range(2):
            at = slot * TILE + 128 * k
            (dp0, dp1)[t % 2][at : at + 128, :] = grads[slot].astype(BF16)
            dt[:, pl.ds(slot * HALF + t * TILE + 128 * k, 128)] = grads[slot].T.astype(BF16)

    def back(t, j):
        dact = dot_t((dp0, dp1)[t % 2][...], w_out_rows(j))
        for slot in range(2):
            at = tile_of(slot, t)
            part = dact[slot * TILE : slot * TILE + TILE]
            slp[j, at, :] = (part * slp[j, at, :].astype(F32)).astype(BF16)

    for t in range(TILES + 1):
        if t < TILES:
            out_tile(t)
        for j in range(4):
            if t > 0:
                back(t - 1, j)
            if t < TILES and j < 2:
                loss_part(t, j)

    mates = [
        sib,
        near,
        pair,
        {Y: y + 1 - 2 * lax.rem(y, 2)},
        {Y: 3 - y},
        {Z: z + 1 - 2 * lax.rem(z, 2)},
        {Z: 3 - z},
    ]

    def loss_copy(n):
        return remote(cr.at[n], crr.at[n], s_cr.at[n], r_cr.at[n], mates[n])

    def loss_next(n):
        loss_copy(n).wait()
        cr[n + 1] = cr[n] + crr[n]
        if n + 1 < len(mates):
            loss_copy(n + 1).start()

    blocks = [lax.rem(z + 2, 4), lax.rem(z + 1, 4), lax.rem(z + 3, 4), z]

    def core_copy(n, s, half):
        j, k = blocks[s], 2 * s + half
        if n == 0:
            at = 2 * j + half
            return remote(si.at[1 - c, at], ri.at[at], s_core.at[0, k], r_core.at[0, k], sib)
        ys = pl.ds(2 * half, 2)
        return remote(so.at[1 - c, j, ys], ro.at[j, ys], s_core.at[1, k], r_core.at[1, k], sib)

    def i_block(s):
        j = blocks[s]
        gi = dot(nt[...], slp[j]).reshape(32, 2, 8, 512)
        for half in range(2):
            for core in range(2):
                part = gi[:, core, :, 256 * half : 256 * half + 256]
                si[core, 2 * j + half] = part.reshape(4, 4, 16, 256).astype(BF16)
        for half in range(2):
            core_copy(0, s, half).start()

    def o_block(s):
        j = blocks[s]
        go = dot(dt[...], act[j]).T.reshape(4, 2, 2, 32, 512)
        for core in range(2):
            so[core, j] = go[:, :, core].reshape(4, 64, 512).astype(BF16)
        for half in range(2):
            core_copy(1, s, half).start()

    def i_add(s):
        for half in range(2):
            core_copy(0, s, half).wait_recv()
            k = 2 * blocks[s] + half
            si[c, k] = (si[c, k].astype(F32) + ri[k].astype(F32)).astype(BF16)

    def o_add(s):
        j = blocks[s]
        for half in range(2):
            core_copy(1, s, half).wait_recv()
            ys = pl.ds(2 * half, 2)
            so[c, j, ys] = (so[c, j, ys].astype(F32) + ro[j, ys].astype(F32)).astype(BF16)

    class Ring:
        def __init__(self, n, axis, view, hr, hq, fr, fq):
            p = place[axis]
            q, r, o = lax.rem(p + 1, 4), lax.rem(p + 3, 4), lax.rem(p + 2, 4)
            self.n, self.axis, self.view, self.p, self.q, self.r = n, axis, view, p, q, r
            self.hr, self.hq, self.fr, self.fq = hr, hq, fr, fq
            self.moves = [
                (view(o, 0), hr, up),
                (view(o, 1), hq, down),
                (view(q, 1), fr.at[1], up),
                (view(r, 0), fq.at[0], down),
                (view(q, 0), fr.at[0], up),
                (view(r, 1), fq.at[1], down),
            ]

        def move(self, k):
            src, dst, who = self.moves[k]
            return remote(src, dst, s_rs.at[self.n, k], r_rs.at[self.n, k], who[self.axis])

        def start(self, *ks):
            for k in ks:
                self.move(k).start()

        def relay(self, k):
            i, part, got = [(self.q, 0, self.hr), (self.r, 1, self.hq)][k]
            self.move(k).wait_recv()
            block = self.view(i, part)
            block[...] = (block[...].astype(F32) + got[...].astype(F32)).astype(BF16)
            self.move(4 + k).start()

        def begin(self):
            self.start(0, 1, 2, 3)

        def middle(self):
            self.relay(0)
            self.relay(1)

        def end(self):
            for k in (2, 3, 4, 5):
                self.move(k).wait_recv()
            return [
                self.view(self.p, part)[...].astype(F32)
                + (self.fr[part].astype(F32) + self.fq[part].astype(F32))
                for part in range(2)
            ]

        def drain(self):
            for k in range(6):
                self.move(k).wait_send()

    class Direct:
        def __init__(self, n, axis, view, got):
            p = place[axis]
            self.view, self.p, self.got = view, p, got
            ends = [(2, away), (1, up), (3, down)]
            self.copies = [
                remote(view(lax.rem(p + d, 4)), got.at[k], s_rs.at[n, k], r_rs.at[n, k], who[axis])
                for k, (d, who) in enumerate(ends)
            ]

        def begin(self):
            for copy in self.copies:
                copy.start()

        def end(self):
            for copy in self.copies:
                copy.wait_recv()
            own, *others = [v.astype(F32) for v in (self.view(self.p)[...], *[self.got[k] for k in range(3)])]
            return (own + others[0]) + (others[1] + others[2])

        def drain(self):
            for copy in self.copies:
                copy.wait_send()

    def i_ring(s):
        return Ring(
            s, Y, lambda i, part: si.at[c, 2 * blocks[s] + part, :, i],
            ihr.at[s], ihq.at[s], ifr.at[s], ifq.at[s],
        )

    i1 = [i_ring(s) for s in range(4)]
    i2 = Direct(4, Z, lambda i: ic.at[:, i], jgot)
    o1 = Ring(5, Z, lambda i, part: so.at[c, i, :, pl.ds(32 * part, 32)], ohr, ohq, ofr, ofq)
    o2 = Direct(6, Y, lambda i: oc.at[i], pgot)

    def i_end(s):
        for part, v in enumerate(i1[s].end()):
            ic[2 * blocks[s] + part] = v.astype(BF16)

    far = {X: 1 - h}

    def x_copies(n, send, got):
        ends = [(near, 1 - h), (far, 1 - h), (pair, h)]
        return [
            remote(send.at[part], got.at[k], s_x.at[n, k], r_x.at[n, k], who)
            for k, (who, part) in enumerate(ends)
        ]

    x_i, x_o = x_copies(0, xi, xir), x_copies(1, xo, xor)

    def x_sum(copies, send, got):
        for copy in copies:
            copy.wait_recv()
        own, beside, across, mate = [v.astype(F32) for v in (send[h], got[0], got[1], got[2])]
        return (own + beside) + (mate + across)

    loss_copy(0).start()
    o_block(0)
    i_block(0)
    o_add(0)
    o1.start(0, 1)
    i_block(1)
    i_add(0)
    i1[0].begin()
    i_block(2)
    i_add(1)
    i1[1].begin()
    i_block(3)
    i_add(2)
    i1[2].begin()
    loss_next(0)
    o_block(1)
    i_add(3)
    i1[3].begin()
    o_block(2)
    o_add(1)
    o1.start(2)
    i1[0].middle()
    o1.relay(0)
    loss_next(1)
    o_block(3)
    o_add(2)
    o1.start(3)
    o1.relay(1)
    i1[1].middle()
    i1[2].middle()
    o_add(3)
    i1[3].middle()
    loss_next(2)
    i_end(0)
    i_end(1)
    i_end(2)
    loss_next(3)
    i_end(3)
    i2.begin()
    for part, v in enumerate(o1.end()):
        oc[:, 32 * part : 32 * part + 32] = v.astype(BF16)
    o2.begin()
    loss_next(4)
    loss_next(5)
    sums = i2.end()
    for half in range(2):
        xi[half] = sums[:, 8 * half : 8 * half + 8].astype(BF16)
    for copy in x_i:
        copy.start()
    sums = o2.end()
    for half in range(2):
        xo[half] = sums[32 * half : 32 * half + 32].astype(BF16)
    for copy in x_o:
        copy.start()
    loss_next(6)
    loss[0, 0] = jnp.sum(cr[7]) * (0.5 / float(2 * NODES * D))
    total = x_sum(x_i, xi, xir)
    for k in range(8):
        g_in[:, 256 * k : 256 * k + 256] = total[k]
    g_out[...] = x_sum(x_o, xo, xor)

    for copy in first_sends + x_i + x_o:
        copy.wait_send()
    for s in range(4):
        gather_drain(s, 0)
        gather_drain(s, 1)
        share(s, c).wait_send()
        for n in range(2):
            for half in range(2):
                core_copy(n, s, half).wait_send()
    for ring in i1 + [i2, o1, o2]:
        ring.drain()
    for t in range(TILES):
        store_own(t).wait()
        send_latents(t).wait_send()
        send_prediction(t).wait_send()
        remote(
            pbuf.at[1, pl.ds(t * TILE, TILE)],
            out.at[0, pl.ds(theirs + t * TILE, TILE)],
            s_prd.at[t],
            r_prd.at[t],
            pair,
        ).wait_recv()


def finish(p_in, gi_in, go_in, p_out, gi_out, go_out, held, gi, go, s_in, s_out):
    routes = [(gi_in, gi, gi_out), (go_in, go, go_out)]
    for k in range(8):
        part = pl.ds(256 * k, 256)
        routes.append((p_in.at[0, part], held.at[part], p_out.at[0, part]))
    loads = [pltpu.make_async_copy(a, b, s_in.at[k]) for k, (a, b, _) in enumerate(routes)]
    stores = [pltpu.make_async_copy(b, d, s_out.at[k]) for k, (_, b, d) in enumerate(routes)]
    for load in loads:
        load.start()
    for load, store in zip(loads, stores):
        load.wait()
        store.start()
    for store in stores:
        store.wait()


def vm(*shape, dtype=BF16):
    return pltpu.VMEM(shape, dtype)


def dma(*shape):
    return pltpu.SemaphoreType.DMA(shape)


SCRATCH = [
    vm(4, 4, 4, 32, 512), vm(4, 4, 4, 128, 128), vm(2, HALF, D), vm(HALF, D), vm(2, HALF, D),
    vm(2, HALF, D), vm(D, ROWS), vm(2 * TILE, D), vm(2 * TILE, D), vm(D, ROWS), vm(4, ROWS, 512), vm(4, ROWS, 512), vm(1, 32, dtype=F32),
    vm(2, 8, 4, 4, 16, 256), vm(2, 4, 4, 64, 512), vm(8, 4, 4, 16, 256), vm(4, 4, 64, 512),
    vm(4, 4, 16, 256), vm(4, 4, 16, 256), vm(4, 2, 4, 16, 256), vm(4, 2, 4, 16, 256),
    vm(4, 32, 512), vm(4, 32, 512), vm(2, 4, 32, 512), vm(2, 4, 32, 512),
    vm(8, 4, 16, 256), vm(4, 64, 512),
    vm(3, 8, 16, 256), vm(3, 64, 512),
    vm(2, 8, 8, 256), vm(3, 8, 8, 256), vm(2, 32, 512), vm(3, 32, 512),
    vm(8, 8, 128, dtype=F32), vm(7, 8, 128, dtype=F32),
    dma(TILES + 1), dma(TILES), dma(TILES), dma(TILES), dma(TILES), dma(TILES),
    pltpu.SemaphoreType.DMA, pltpu.SemaphoreType.DMA,
    dma(3, 4), dma(3, 4), dma(4), dma(4, 2, 4), dma(4, 2, 4), dma(4), dma(4), dma(2, 8), dma(2, 8),
    dma(7, 6), dma(7, 6), dma(2, 3), dma(2, 3), dma(7), dma(7),
]


def on_device(latents, noise, cond_gain, cond_shift, w_in, b_in, w_out, target):
    inside = pl.BlockSpec(memory_space=pltpu.VMEM)
    anywhere = pl.BlockSpec(memory_space=pl.ANY)
    prediction, grad_in, grad_out, loss = pl.pallas_call(
        kernel,
        out_shape=(
            jax.ShapeDtypeStruct((1, ROWS, D), BF16),
            jax.ShapeDtypeStruct((8, H), F32),
            jax.ShapeDtypeStruct((32, D), F32),
            jax.ShapeDtypeStruct((1, 1), F32),
        ),
        in_specs=[anywhere] + [inside] * 6 + [anywhere],
        out_specs=(anywhere, inside, inside, pl.BlockSpec(memory_space=pltpu.SMEM)),
        scratch_shapes=SCRATCH,
        compiler_params=pltpu.CompilerParams(
            collective_id=0, has_side_effects=True, vmem_limit_bytes=63 * 1024 * 1024
        ),
    )(latents, noise, cond_gain, cond_shift, w_in, b_in.reshape(1, H), w_out, target)
    prediction, grad_in, grad_out = pl.pallas_call(
        finish,
        out_shape=(
            jax.ShapeDtypeStruct((1, ROWS, D), BF16),
            jax.ShapeDtypeStruct((8, H), F32),
            jax.ShapeDtypeStruct((32, D), F32),
        ),
        in_specs=[anywhere] * 3,
        out_specs=(anywhere,) * 3,
        scratch_shapes=[vm(ROWS, D), vm(8, H, dtype=F32), vm(32, D, dtype=F32), dma(10), dma(10)],
    )(prediction, grad_in, grad_out)
    return prediction, grad_in, grad_out, loss.reshape(())


def solution(mesh):
    torus = Mesh(mesh.devices.reshape(2, 4, 4, 2, 2), AXES)
    in_specs = (
        P(M, FSDP, None),
        P(M, None),
        P(),
        P(),
        P(FSDP, None),
        P(),
        P(FSDP, None),
        P(FSDP, None),
    )
    out_specs = (P(M, FSDP, None), P(FSDP, None), P(FSDP, None), P())
    return jax.shard_map(on_device, mesh=torus, in_specs=in_specs, out_specs=out_specs, check_vma=False)
```

```python
import jax
import jax.numpy as jnp
from jax import lax
from jax.experimental import pallas as pl
from jax.experimental.pallas import tpu as pltpu
from jax.sharding import Mesh
from jax.sharding import PartitionSpec as P

M, Z, Y, X, C = AXES = ("member", "fsdp_0", "fsdp_1", "fsdp_2", "fsdp_3")
FSDP = (Z, Y, X, C)
MESH = pl.DeviceIdType.MESH
F32 = jnp.float32
BF16 = jnp.bfloat16

COEF = 0.7978845608
CUBIC = 0.044715

D = 512
H = 2048
ROWS = 2048
HALF = 1024
NODES = 131072
TILE = 256
TILES = HALF // TILE


def remote(src, dst, send, recv, device):
    return pltpu.make_async_remote_copy(
        src_ref=src, dst_ref=dst, send_sem=send, recv_sem=recv, device_id=device, device_id_type=MESH
    )


def dot(a, b):
    return jnp.dot(a, b, preferred_element_type=F32)


def dot_t(a, b):
    return lax.dot_general(a, b, (((1,), (1,)), ((), ())), preferred_element_type=F32)


def gain_of(noise, cond):
    n = noise.shape[1]
    square = (n, n)
    same = lax.broadcasted_iota(jnp.int32, square, 0) == lax.broadcasted_iota(jnp.int32, square, 1)
    column = jnp.sum(jnp.where(same, jnp.broadcast_to(noise, square), 0.0), axis=1, keepdims=True)
    return jnp.sum(column * cond, axis=0, keepdims=True)


def kernel(
    latents, noise, cond_gain, cond_shift, w_in, b_in, w_out, target,
    out, g_in, g_out, loss,
    wi, wo, lat, tgt, pbuf, nrm, nt, dp0, dp1, dt, act, slp, nz,
    si, so, ri, ro, ihr, ihq, ifr, ifq, ohr, ohq, ofr, ofq,
    ic, oc, jgot, pgot, lgot,
    xi, xir, xo, xor, cr, crr,
    s_ld, s_out, s_lat, r_lat, s_prd, r_prd, s_nz, r_nz,
    s_w0, r_w0, l_w0, s_ag, r_ag, s_sib, r_sib, s_core, r_core, s_rs, r_rs, s_x, r_x, s_cr, r_cr,
):
    m, z, y, h, c = [lax.axis_index(a) for a in AXES]
    up = {Y: {Y: lax.rem(y + 1, 4)}, Z: {Z: lax.rem(z + 1, 4)}}
    down = {Y: {Y: lax.rem(y + 3, 4)}, Z: {Z: lax.rem(z + 3, 4)}}
    away = {Y: {Y: lax.rem(y + 2, 4)}, Z: {Z: lax.rem(z + 2, 4)}}
    place = {Y: y, Z: z}
    sib = {C: 1 - c}
    pair = {M: 1 - m}
    near = {X: 1 - h, M: 1 - m}
    cross = {X: 1 - h, M: 1 - m, C: 1 - c}

    mine, theirs = m * HALF, (1 - m) * HALF

    def load_own(t):
        return pltpu.make_async_copy(
            latents.at[0, pl.ds(mine + t * TILE, TILE)], lat.at[0, pl.ds(t * TILE, TILE)], s_ld.at[t]
        )

    load_target = pltpu.make_async_copy(target.at[pl.ds(mine, HALF)], tgt, s_ld.at[TILES])
    for t in range(TILES):
        load_own(t).start()
    load_target.start()

    barrier = pltpu.get_barrier_semaphore()
    greeted = [sib, pair, near, cross, {X: 1 - h}, away[Y], away[Z], up[Y], down[Y], up[Z], down[Z]]
    for other in greeted:
        pl.semaphore_signal(barrier, inc=1, device_id=other, device_id_type=MESH)
    pl.semaphore_wait(barrier, len(greeted))

    def shard_parts(h_from, c_from, c_to):
        row = 2 * h_from + c_from
        parts = []
        for k in range(2):
            col = pl.ds(pl.multiple_of(c_to * 1024 + k * 512, 512), 512)
            parts.append((w_in.at[:, col], wi.at[2 * c_to + k, z, y, pl.ds(8 * row, 8)]))
        for k in range(2):
            col = pl.ds(pl.multiple_of(c_to * 256 + k * 128, 128), 128)
            parts.append((w_out.at[:, col], wo.at[2 * c_to + k, z, y, pl.ds(32 * row, 32)]))
        return parts

    partners = [(near, 1 - h, c), (cross, 1 - h, 1 - c), (sib, h, 1 - c)]
    first_sends = []
    for n, (src, dst) in enumerate(shard_parts(h, c, c)):
        pltpu.make_async_copy(src, dst, l_w0.at[n]).start()
    for n in range(4):
        for r, (who, _, c_to) in enumerate(partners):
            src, dst = shard_parts(h, c, c_to)[n]
            copy = remote(src, dst, s_w0.at[r, n], r_w0.at[r, n], who)
            copy.start()
            first_sends.append(copy)

    noise_copy = remote(noise, nz, s_nz, r_nz, pair)
    noise_copy.start()

    def send_latents(t):
        return remote(
            latents.at[0, pl.ds(theirs + t * TILE, TILE)],
            lat.at[1, pl.ds(t * TILE, TILE)],
            s_lat.at[t],
            r_lat.at[t],
            pair,
        )

    for t in range(TILES):
        send_latents(t).start()

    def tile_of(slot, t):
        return pl.ds(pl.multiple_of(slot * HALF + t * TILE, TILE), TILE)

    def normalise(slot, t, gain, shift):
        if slot == 0:
            load_own(t).wait()
        else:
            send_latents(t).wait_recv()
        x = lat[slot, tile_of(0, t), :].astype(F32)
        centred = x - jnp.mean(x, axis=1, keepdims=True)
        spread = jnp.mean(centred * centred, axis=1, keepdims=True)
        normed = centred * lax.rsqrt(spread + 0.25) * gain + shift
        nt[:, tile_of(slot, t)] = normed.T.astype(BF16)
        nrm[slot, tile_of(0, t), :] = normed.astype(BF16)

    gain, shift = 1.0 + gain_of(noise[...], cond_gain[...]), gain_of(noise[...], cond_shift[...])
    for t in range(2):
        normalise(0, t, gain, shift)
    streams = [(wi, 0, Y), (wi, 1, Z), (wo, 0, Y), (wo, 1, Z)]

    def other_axis(a):
        return Z if a == Y else Y

    def gather_view(s, phase, i, part):
        ref, k, first = streams[s]
        size = ref.shape[3]
        rows = pl.ds(0, size) if part is None else pl.ds(part * size // 2, size // 2)
        block = 2 * c + k
        if phase == 0:
            return ref.at[block, z, i, rows] if first == Y else ref.at[block, i, y, rows]
        return ref.at[block, i, :, rows] if first == Y else ref.at[block, :, i, rows]

    def gather_copy(s, phase, n):
        axis = streams[s][2] if phase == 0 else other_axis(streams[s][2])
        p = place[axis]
        if phase == 0:
            i, part, who = p, None, [up, down, away][n][axis]
        else:
            i = [p, p, lax.rem(p + 3, 4), lax.rem(p + 1, 4)][n]
            part, who = [None, None, 0, 1][n], [up, down, up, down][n][axis]
        view = gather_view(s, phase, i, part)
        return remote(view, view, s_ag.at[s, phase, n], r_ag.at[s, phase, n], who)

    def gather_landed(s, phase, n):
        axis = streams[s][2] if phase == 0 else other_axis(streams[s][2])
        p = place[axis]
        i = lax.rem(p + [3, 1, 2, 2][n], 4)
        view = gather_view(s, phase, i, None if phase == 0 else [None, None, 0, 1][n])
        remote(view, view, s_ag.at[s, phase, n], r_ag.at[s, phase, n], up[axis]).wait_recv()

    def gather_start(s, phase):
        for n in range(3 if phase == 0 else 2):
            gather_copy(s, phase, n).start()

    def gather_forward(s, phase):
        if phase == 0:
            return
        gather_landed(s, phase, 0)
        gather_copy(s, phase, 2).start()
        gather_landed(s, phase, 1)
        gather_copy(s, phase, 3).start()

    def gather_end(s, phase):
        for n in range(3) if phase == 0 else (2, 3):
            gather_landed(s, phase, n)

    def gather_drain(s, phase):
        for n in range(3 if phase == 0 else 4):
            gather_copy(s, phase, n).wait_send()

    def share(s, block_of):
        ref, k, _ = streams[s]
        view = ref.at[2 * block_of + k]
        return remote(view, view, s_sib.at[s], r_sib.at[s], sib)

    for n in range(4):
        src, dst = shard_parts(h, c, c)[n]
        pltpu.make_async_copy(src, dst, l_w0.at[n]).wait()
        for r, (who, h_from, c_from) in enumerate(partners):
            src, dst = shard_parts(h_from, c_from, c)[n]
            remote(src, dst, s_w0.at[r, n], r_w0.at[r, n], who).wait_recv()
        gather_start(n, 0)
    normalise(0, 2, gain, shift)
    for s in range(4):
        gather_forward(s, 0)
    normalise(0, 3, gain, shift)
    for s in range(2):
        gather_end(s, 0)
        gather_start(s, 1)
    noise_copy.wait()
    other_gain, other_shift = 1.0 + gain_of(nz[...], cond_gain[...]), gain_of(nz[...], cond_shift[...])
    normalise(1, 0, other_gain, other_shift)
    for s in range(2):
        gather_forward(s, 1)
    for s in range(2, 4):
        gather_end(s, 0)
        gather_start(s, 1)
    normalise(1, 1, other_gain, other_shift)
    for s in range(2):
        gather_end(s, 1)
        share(s, c).start()
    for s in range(2):
        share(s, 1 - c).wait_recv()

    def w_out_rows(j):
        return jnp.concatenate([wo[b, j].reshape(512, 128) for b in range(4)], axis=1)

    def hidden(j, slot, t):
        rows = tile_of(slot, t)
        v = dot(nrm[slot, tile_of(0, t), :], wi[j].reshape(512, 512)) + b_in[:, 512 * j : 512 * j + 512]
        q = v * v
        u = jnp.tanh(v * (COEF + (COEF * CUBIC) * q))
        half = 0.5 + 0.5 * u
        a = v * half
        slope = half + a * ((1.0 - half) * (2.0 * COEF + (6.0 * COEF * CUBIC) * q))
        a = a.astype(BF16)
        act[j, rows, :] = a
        slp[j, rows, :] = slope.astype(BF16)
        return a

    def store_own(t):
        return pltpu.make_async_copy(
            pbuf.at[0, pl.ds(t * TILE, TILE)], out.at[0, pl.ds(mine + t * TILE, TILE)], s_out.at[t]
        )

    def send_prediction(t):
        return remote(
            pbuf.at[1, pl.ds(t * TILE, TILE)],
            out.at[0, pl.ds(mine + t * TILE, TILE)],
            s_prd.at[t],
            r_prd.at[t],
            pair,
        )

    def own_hidden(t, carry):
        for j in range(4):
            hidden(j, 0, t)
        return carry

    def partner_hidden(t, carry):
        for j in range(4):
            hidden(j, 1, t)
        return carry

    def own_out(t, beside):
        x = lat[0, tile_of(0, t), :].astype(F32)
        for j in range(4):
            x = x + dot(act[j, tile_of(0, t), :], w_out_rows(j))
            if beside is not None:
                hidden(j, 1, beside)
        pbuf[0, tile_of(0, t), :] = x.astype(BF16)
        store_own(t).start()

    lax.fori_loop(0, 1, own_hidden, 0)
    for s in range(2, 4):
        gather_forward(s, 1)
    lax.fori_loop(1, TILES, own_hidden, 0)
    for t in range(2, TILES):
        normalise(1, t, other_gain, other_shift)
    for s in range(2, 4):
        gather_end(s, 1)
        share(s, c).start()
    lax.fori_loop(0, 2, partner_hidden, 0)
    for s in range(2, 4):
        share(s, 1 - c).wait_recv()
    for t in range(TILES):
        own_out(t, t + 2 if t + 2 < TILES else None)

    load_target.wait()
    cr[0] = jnp.zeros((8, 128), F32)
    scale = float((2 * NODES) ** -0.5)

    def out_tile(t):
        x = lat[1, tile_of(0, t), :].astype(F32)
        for j in range(4):
            x = x + dot(act[j, tile_of(1, t), :], w_out_rows(j))
        pbuf[1, tile_of(0, t), :] = x.astype(BF16)
        send_prediction(t).start()

    def loss_part(t, k):
        rows = pl.ds(t * TILE + 128 * k, 128)
        p0 = pbuf[0, rows, :].astype(F32)
        p1 = pbuf[1, rows, :].astype(F32)
        goal = tgt[rows, :].astype(F32)
        near0, near1, apart = p0 - goal, p1 - goal, p0 - p1
        q0, q1, qa = near0 * near0 + 0.0625, near1 * near1 + 0.0625, apart * apart + 0.0625
        i0, i1, ia = lax.rsqrt(q0), lax.rsqrt(q1), lax.rsqrt(qa)
        crps = q0 * i0 + q1 * i1 - qa * ia
        summed = jnp.sum(crps.reshape(16, 8, D), axis=0)
        cr[0] += sum(summed[:, n * 128 : (n + 1) * 128] for n in range(4))
        pull = (0.5 * scale) * (apart * ia)
        grads = ((0.5 * scale) * (near0 * i0) - pull, (0.5 * scale) * (near1 * i1) + pull)
        for slot in range(2):
            at = slot * TILE + 128 * k
            (dp0, dp1)[t % 2][at : at + 128, :] = grads[slot].astype(BF16)
            dt[:, pl.ds(slot * HALF + t * TILE + 128 * k, 128)] = grads[slot].T.astype(BF16)

    def back(t, j):
        dact = dot_t((dp0, dp1)[t % 2][...], w_out_rows(j))
        for slot in range(2):
            at = tile_of(slot, t)
            part = dact[slot * TILE : slot * TILE + TILE]
            slp[j, at, :] = (part * slp[j, at, :].astype(F32)).astype(BF16)

    for t in range(TILES + 1):
        if t < TILES:
            out_tile(t)
        for j in range(4):
            if t > 0:
                back(t - 1, j)
            if t < TILES and j < 2:
                loss_part(t, j)

    mates = [
        sib,
        near,
        pair,
        {Y: y + 1 - 2 * lax.rem(y, 2)},
        {Y: 3 - y},
        {Z: z + 1 - 2 * lax.rem(z, 2)},
        {Z: 3 - z},
    ]

    def loss_copy(n):
        return remote(cr.at[n], crr.at[n], s_cr.at[n], r_cr.at[n], mates[n])

    def loss_next(n):
        loss_copy(n).wait()
        cr[n + 1] = cr[n] + crr[n]
        if n + 1 < len(mates):
            loss_copy(n + 1).start()

    blocks = [lax.rem(z + 2, 4), lax.rem(z + 1, 4), lax.rem(z + 3, 4), z]

    def core_copy(n, s, half):
        j, k = blocks[s], 2 * s + half
        if n == 0:
            at = 2 * j + half
            return remote(si.at[1 - c, at], ri.at[at], s_core.at[0, k], r_core.at[0, k], sib)
        ys = pl.ds(2 * half, 2)
        return remote(so.at[1 - c, j, ys], ro.at[j, ys], s_core.at[1, k], r_core.at[1, k], sib)

    def i_block(s):
        j = blocks[s]
        gi = dot(nt[...], slp[j]).reshape(32, 2, 8, 512)
        for half in range(2):
            for core in range(2):
                part = gi[:, core, :, 256 * half : 256 * half + 256]
                si[core, 2 * j + half] = part.reshape(4, 4, 16, 256).astype(BF16)
        for half in range(2):
            core_copy(0, s, half).start()

    def o_block(s):
        j = blocks[s]
        go = dot(dt[...], act[j]).T.reshape(4, 2, 2, 32, 512)
        for core in range(2):
            so[core, j] = go[:, :, core].reshape(4, 64, 512).astype(BF16)
        for half in range(2):
            core_copy(1, s, half).start()

    def i_add(s):
        for half in range(2):
            core_copy(0, s, half).wait_recv()
            k = 2 * blocks[s] + half
            si[c, k] = (si[c, k].astype(F32) + ri[k].astype(F32)).astype(BF16)

    def o_add(s):
        j = blocks[s]
        for half in range(2):
            core_copy(1, s, half).wait_recv()
            ys = pl.ds(2 * half, 2)
            so[c, j, ys] = (so[c, j, ys].astype(F32) + ro[j, ys].astype(F32)).astype(BF16)

    class Ring:
        def __init__(self, n, axis, view, hr, hq, fr, fq):
            p = place[axis]
            q, r, o = lax.rem(p + 1, 4), lax.rem(p + 3, 4), lax.rem(p + 2, 4)
            self.n, self.axis, self.view, self.p, self.q, self.r = n, axis, view, p, q, r
            self.hr, self.hq, self.fr, self.fq = hr, hq, fr, fq
            self.moves = [
                (view(o, 0), hr, up),
                (view(o, 1), hq, down),
                (view(q, 1), fr.at[1], up),
                (view(r, 0), fq.at[0], down),
                (view(q, 0), fr.at[0], up),
                (view(r, 1), fq.at[1], down),
            ]

        def move(self, k):
            src, dst, who = self.moves[k]
            return remote(src, dst, s_rs.at[self.n, k], r_rs.at[self.n, k], who[self.axis])

        def start(self, *ks):
            for k in ks:
                self.move(k).start()

        def relay(self, k):
            i, part, got = [(self.q, 0, self.hr), (self.r, 1, self.hq)][k]
            self.move(k).wait_recv()
            block = self.view(i, part)
            block[...] = (block[...].astype(F32) + got[...].astype(F32)).astype(BF16)
            self.move(4 + k).start()

        def begin(self):
            self.start(0, 1, 2, 3)

        def middle(self):
            self.relay(0)
            self.relay(1)

        def end(self):
            for k in (2, 3, 4, 5):
                self.move(k).wait_recv()
            return [
                self.view(self.p, part)[...].astype(F32)
                + (self.fr[part].astype(F32) + self.fq[part].astype(F32))
                for part in range(2)
            ]

        def drain(self):
            for k in range(6):
                self.move(k).wait_send()

    class Direct:
        def __init__(self, n, axis, view, got):
            p = place[axis]
            self.view, self.p, self.got = view, p, got
            ends = [(2, away), (1, up), (3, down)]
            self.copies = [
                remote(view(lax.rem(p + d, 4)), got.at[k], s_rs.at[n, k], r_rs.at[n, k], who[axis])
                for k, (d, who) in enumerate(ends)
            ]

        def begin(self):
            for copy in self.copies:
                copy.start()

        def end(self):
            for copy in self.copies:
                copy.wait_recv()
            own, *others = [v.astype(F32) for v in (self.view(self.p)[...], *[self.got[k] for k in range(3)])]
            return (own + others[0]) + (others[1] + others[2])

        def drain(self):
            for copy in self.copies:
                copy.wait_send()

    def i_ring(s):
        return Ring(
            s, Y, lambda i, part: si.at[c, 2 * blocks[s] + part, :, i],
            ihr.at[s], ihq.at[s], ifr.at[s], ifq.at[s],
        )

    i1 = [i_ring(s) for s in range(3)]
    i1.append(Direct(3, Y, lambda i: si.at[c, pl.ds(2 * blocks[3], 2), :, i], lgot))
    i2 = Direct(4, Z, lambda i: ic.at[:, i], jgot)
    o1 = Ring(5, Z, lambda i, part: so.at[c, i, :, pl.ds(32 * part, 32)], ohr, ohq, ofr, ofq)
    o2 = Direct(6, Y, lambda i: oc.at[i], pgot)

    def i_end(s):
        sums = i1[s].end()
        for part in range(2):
            ic[2 * blocks[s] + part] = sums[part].astype(BF16)

    far = {X: 1 - h}

    def x_copies(n, send, got):
        ends = [(near, 1 - h), (far, 1 - h), (pair, h)]
        return [
            remote(send.at[part], got.at[k], s_x.at[n, k], r_x.at[n, k], who)
            for k, (who, part) in enumerate(ends)
        ]

    x_i, x_o = x_copies(0, xi, xir), x_copies(1, xo, xor)

    def x_sum(copies, send, got):
        for copy in copies:
            copy.wait_recv()
        own, beside, across, mate = [v.astype(F32) for v in (send[h], got[0], got[1], got[2])]
        return (own + beside) + (mate + across)

    loss_copy(0).start()
    o_block(0)
    i_block(0)
    o_add(0)
    o1.start(0, 1)
    i_block(1)
    i_add(0)
    i1[0].begin()
    i_block(2)
    i_add(1)
    i1[1].begin()
    o_block(1)
    i_add(2)
    i1[2].begin()
    loss_next(0)
    o_block(2)
    o_add(1)
    o1.start(2)
    i_block(3)
    o_add(2)
    o1.start(3)
    i1[0].middle()
    o1.relay(0)
    loss_next(1)
    o_block(3)
    i_add(3)
    i1[3].begin()
    o1.relay(1)
    i1[1].middle()
    i1[2].middle()
    o_add(3)
    loss_next(2)
    i_end(0)
    i_end(1)
    i_end(2)
    loss_next(3)
    i_end(3)
    i2.begin()
    for part, v in enumerate(o1.end()):
        oc[:, 32 * part : 32 * part + 32] = v.astype(BF16)
    o2.begin()
    loss_next(4)
    loss_next(5)
    sums = i2.end()
    for half in range(2):
        xi[half] = sums[:, 8 * half : 8 * half + 8].astype(BF16)
    for copy in x_i:
        copy.start()
    sums = o2.end()
    for half in range(2):
        xo[half] = sums[32 * half : 32 * half + 32].astype(BF16)
    for copy in x_o:
        copy.start()
    loss_next(6)
    loss[0, 0] = jnp.sum(cr[7]) * (0.5 / float(2 * NODES * D))
    total = x_sum(x_i, xi, xir)
    for k in range(8):
        g_in[:, 256 * k : 256 * k + 256] = total[k]
    g_out[...] = x_sum(x_o, xo, xor)

    for copy in first_sends + x_i + x_o:
        copy.wait_send()
    for s in range(4):
        gather_drain(s, 0)
        gather_drain(s, 1)
        share(s, c).wait_send()
        for n in range(2):
            for half in range(2):
                core_copy(n, s, half).wait_send()
    for ring in i1 + [i2, o1, o2]:
        ring.drain()
    for t in range(TILES):
        store_own(t).wait()
        send_latents(t).wait_send()
        send_prediction(t).wait_send()
        remote(
            pbuf.at[1, pl.ds(t * TILE, TILE)],
            out.at[0, pl.ds(theirs + t * TILE, TILE)],
            s_prd.at[t],
            r_prd.at[t],
            pair,
        ).wait_recv()


def finish(p_in, gi_in, go_in, p_out, gi_out, go_out, held, gi, go, s_in, s_out):
    routes = [(gi_in, gi, gi_out), (go_in, go, go_out)]
    for k in range(8):
        part = pl.ds(256 * k, 256)
        routes.append((p_in.at[0, part], held.at[part], p_out.at[0, part]))
    loads = [pltpu.make_async_copy(a, b, s_in.at[k]) for k, (a, b, _) in enumerate(routes)]
    stores = [pltpu.make_async_copy(b, d, s_out.at[k]) for k, (_, b, d) in enumerate(routes)]
    for load in loads:
        load.start()
    for load, store in zip(loads, stores):
        load.wait()
        store.start()
    for store in stores:
        store.wait()


def vm(*shape, dtype=BF16):
    return pltpu.VMEM(shape, dtype)


def dma(*shape):
    return pltpu.SemaphoreType.DMA(shape)


SCRATCH = [
    vm(4, 4, 4, 32, 512), vm(4, 4, 4, 128, 128), vm(2, HALF, D), vm(HALF, D), vm(2, HALF, D),
    vm(2, HALF, D), vm(D, ROWS), vm(2 * TILE, D), vm(2 * TILE, D), vm(D, ROWS), vm(4, ROWS, 512), vm(4, ROWS, 512), vm(1, 32, dtype=F32),
    vm(2, 8, 4, 4, 16, 256), vm(2, 4, 4, 64, 512), vm(8, 4, 4, 16, 256), vm(4, 4, 64, 512),
    vm(4, 4, 16, 256), vm(4, 4, 16, 256), vm(4, 2, 4, 16, 256), vm(4, 2, 4, 16, 256),
    vm(4, 32, 512), vm(4, 32, 512), vm(2, 4, 32, 512), vm(2, 4, 32, 512),
    vm(8, 4, 16, 256), vm(4, 64, 512),
    vm(3, 8, 16, 256), vm(3, 64, 512), vm(3, 2, 4, 16, 256),
    vm(2, 8, 8, 256), vm(3, 8, 8, 256), vm(2, 32, 512), vm(3, 32, 512),
    vm(8, 8, 128, dtype=F32), vm(7, 8, 128, dtype=F32),
    dma(TILES + 1), dma(TILES), dma(TILES), dma(TILES), dma(TILES), dma(TILES),
    pltpu.SemaphoreType.DMA, pltpu.SemaphoreType.DMA,
    dma(3, 4), dma(3, 4), dma(4), dma(4, 2, 4), dma(4, 2, 4), dma(4), dma(4), dma(2, 8), dma(2, 8),
    dma(7, 6), dma(7, 6), dma(2, 3), dma(2, 3), dma(7), dma(7),
]


def on_device(latents, noise, cond_gain, cond_shift, w_in, b_in, w_out, target):
    inside = pl.BlockSpec(memory_space=pltpu.VMEM)
    anywhere = pl.BlockSpec(memory_space=pl.ANY)
    prediction, grad_in, grad_out, loss = pl.pallas_call(
        kernel,
        out_shape=(
            jax.ShapeDtypeStruct((1, ROWS, D), BF16),
            jax.ShapeDtypeStruct((8, H), F32),
            jax.ShapeDtypeStruct((32, D), F32),
            jax.ShapeDtypeStruct((1, 1), F32),
        ),
        in_specs=[anywhere] + [inside] * 6 + [anywhere],
        out_specs=(anywhere, inside, inside, pl.BlockSpec(memory_space=pltpu.SMEM)),
        scratch_shapes=SCRATCH,
        compiler_params=pltpu.CompilerParams(
            collective_id=0, has_side_effects=True, vmem_limit_bytes=63 * 1024 * 1024
        ),
    )(latents, noise, cond_gain, cond_shift, w_in, b_in.reshape(1, H), w_out, target)
    prediction, grad_in, grad_out = pl.pallas_call(
        finish,
        out_shape=(
            jax.ShapeDtypeStruct((1, ROWS, D), BF16),
            jax.ShapeDtypeStruct((8, H), F32),
            jax.ShapeDtypeStruct((32, D), F32),
        ),
        in_specs=[anywhere] * 3,
        out_specs=(anywhere,) * 3,
        scratch_shapes=[vm(ROWS, D), vm(8, H, dtype=F32), vm(32, D, dtype=F32), dma(10), dma(10)],
    )(prediction, grad_in, grad_out)
    return prediction, grad_in, grad_out, loss.reshape(())


def solution(mesh):
    torus = Mesh(mesh.devices.reshape(2, 4, 4, 2, 2), AXES)
    in_specs = (
        P(M, FSDP, None),
        P(M, None),
        P(),
        P(),
        P(FSDP, None),
        P(),
        P(FSDP, None),
        P(FSDP, None),
    )
    out_specs = (P(M, FSDP, None), P(FSDP, None), P(FSDP, None), P())
    return jax.shard_map(on_device, mesh=torus, in_specs=in_specs, out_specs=out_specs, check_vma=False)
```
